32 devices in a mesh: cfg: 2 (over x), seq: 16 (over z, y, core).
Axes of the slice: x: 2, y: 2, z: 4, core: 2. Of those that a mesh axis runs over, the one named last changes fastest.
Arguments:
- hidden: bfloat16 [2, 2048, 1920], P('cfg', 'seq'), may hold values from -6 to 6
- modulation: float32 [6, 1920], replicated, may hold values from -3 to 3
- w_qkv: bfloat16 [3, 1920, 1024], replicated, may hold values from -0.125 to 0.125
- q_gain: float32 [64], replicated, may hold values from 1 to 13, as said below
- k_gain: float32 [64], replicated, may hold values from 1 to 13, as said below
- w_out: bfloat16 [1024, 1920], replicated, may hold values from -0.1875 to 0.1875
- text_count: int32 [2], P('cfg'), may hold values from 1 to 226
- block_order: int32 [16], P('seq'), may hold values from 0 to 15, each once
Outputs:
- guided: float32 [2048, 1920], P('seq', 'cfg')
The draws below stay inside these ranges and needn't reach their ends.
Inputs may be any that keep to these rules, and one draw needn't show every extreme that they name: text_count[b] is how many of the 226 text positions of branch b (0 conditional, 1 unconditional) hold prompt tokens; keys at the other text positions are masked. Seq index j holds positions block_order[j] * 128 to block_order[j] * 128 + 127; every block appears once. `q_gain`: one gain for each of the 64 entries of a head, shared by all heads. `k_gain`: one gain for each of the 64 entries of a head, shared by all heads.
All inputs are finite; a program needn't handle non-finite values.
Results may differ from the reference program's by a relative error of at most 0.015.
The reference program's roundings to bfloat16 on the way (of `modded`, `key_bias`, `weights` and `attended`) count: a program that leaves them out, or rounds other values in their place, can miss the bound.
Values may be sent and summed in bfloat16 or wider, within the bound.
A program may use at most 256 MiB of HBM per device.

```python
import math
import jax
import jax.numpy as jnp
from jax import lax

D = 1920
HEAD = 64
HEADS = 16
TOK_DEV = 128
TXT = 226
TOKENS = 2048
N_SEQ = 16


def norm_gain(key, member):
    large_count = 3
    large_low = 7.0
    large_high = 9.0
    ranking = jax.random.permutation(jax.random.fold_in(key, 9001), HEAD)
    chosen = ranking < large_count
    member_key = jax.random.fold_in(key, member)
    base_gain = jnp.exp(jax.random.uniform(jax.random.fold_in(member_key, 1), (HEAD,), jnp.float32, 0.0, math.log(2.2)))
    large_gain = jax.random.uniform(jax.random.fold_in(member_key, 2), (HEAD,), jnp.float32, large_low, large_high)
    return jnp.where(chosen, large_gain, base_gain).astype(jnp.float32)


def draw_q_gain(key, part):
    return norm_gain(key, 11)


def draw_k_gain(key, part):
    return norm_gain(key, 23)


def steps_of(rng, extent, cuts, smallest, high):
    loudness, own = 1.0, jax.random.fold_in(rng, 6)
    for dim, parts in cuts:
        heights = jnp.exp(jax.random.uniform(jax.random.fold_in(own, dim), (parts,), jnp.float32, smallest / len(cuts), high / len(cuts)))
        loudness = loudness * jnp.repeat(heights, extent[dim] // parts).reshape([-1 if axis == dim else 1 for axis in range(len(extent))])
    return loudness


def gaussian(key, dims, scale, most, split=(), kind=jnp.bfloat16):
    loudness = steps_of(key, dims, split, -0.22, 0.18) if split else 1.0
    drawn = jax.random.normal(key, dims, jnp.float32) * scale * loudness
    return jnp.minimum(jnp.maximum(drawn, -most), most).astype(kind)


def setup_inputs(seed: int = 0) -> dict:
    key_list = jax.random.split(jax.random.key(seed), 9)
    return {
        "hidden": gaussian(key_list[0], (2, TOKENS, D), 1.0, 6.0, ((0, 2), (1, 16))),
        "modulation": gaussian(key_list[1], (6, D), 0.5, 3.0, (), jnp.float32),
        "w_qkv": gaussian(key_list[2], (3, D, HEADS * HEAD), D ** -0.5, 0.125),
        "q_gain": draw_q_gain(jax.random.fold_in(key_list[8], 71), 0),
        "k_gain": draw_k_gain(jax.random.fold_in(key_list[8], 71), 0),
        "w_out": gaussian(key_list[5], (HEADS * HEAD, D), (HEADS * HEAD) ** -0.5, 0.1875),
        "text_count": jax.random.randint(key_list[6], (2,), 1, TXT + 1).astype(jnp.int32),
        "block_order": jax.random.permutation(key_list[7], N_SEQ).astype(jnp.int32),
    }


GUIDANCE = 6.0
EPSILON = 1e-05
MASKED = -1000000000.0

def layer_normal(values_in):
    average = lax.optimization_barrier(jnp.mean(values_in, axis=-1, keepdims=True))
    centred = values_in - average
    spread = lax.optimization_barrier(jnp.mean(centred * centred, axis=-1, keepdims=True))
    return centred * lax.rsqrt(spread + EPSILON)

def modulated(states, is_text, modulation):
    normed = layer_normal(states.astype(jnp.float32))
    shift = jnp.where(is_text[:, None], modulation[3][None, :], modulation[0][None, :])
    scale = jnp.where(is_text[:, None], modulation[4][None, :], modulation[1][None, :])
    return (normed * (1.0 + scale) + shift).astype(jnp.bfloat16)

def head_normal(projected, gain):
    rows = projected.shape[0]
    heads_view = projected.reshape(rows, HEADS, HEAD)
    return (layer_normal(heads_view) * gain).reshape(rows, HEADS * HEAD).astype(jnp.bfloat16)

def projections(states, is_text, modulation, w_qkv, q_gain, k_gain):
    modded = modulated(states, is_text, modulation)
    query = head_normal(jnp.dot(modded, w_qkv[0], preferred_element_type=jnp.float32), q_gain)
    keys = head_normal(jnp.dot(modded, w_qkv[1], preferred_element_type=jnp.float32), k_gain)
    values = jnp.dot(modded, w_qkv[2], preferred_element_type=jnp.float32).astype(jnp.bfloat16)
    return (query, keys, values)

def attend_block(query_block, key_heads, value_heads, bias_wide):
    rows = query_block.shape[0]
    query_heads = query_block.astype(jnp.float32).reshape(rows, HEADS, HEAD)
    scores = jnp.einsum('qhd,khd->hqk', query_heads, key_heads) * HEAD ** (-0.5) + bias_wide[None, None, :]
    highest = lax.optimization_barrier(jnp.max(scores, axis=-1, keepdims=True))
    expo = jnp.exp(scores - highest)
    total = lax.optimization_barrier(jnp.sum(expo, axis=-1))
    weights = expo.astype(jnp.bfloat16).astype(jnp.float32)
    numer = jnp.einsum('hqk,khd->qhd', weights, value_heads)
    return (numer / total.T[:, :, None]).reshape(rows, HEADS * HEAD).astype(jnp.bfloat16)

def reference(hidden, modulation, w_qkv, q_gain, k_gain, w_out, text_count, block_order):
    within = jnp.arange(TOK_DEV, dtype=jnp.int32)
    position = (block_order[:, None].astype(jnp.int32) * TOK_DEV + within[None, :]).reshape(TOKENS)
    is_text = position < TXT
    gate = jnp.where(is_text[:, None], modulation[5][None, :], modulation[2][None, :])
    query_rows = 512 if TOKENS % 512 == 0 else TOKENS

    def one_branch(states, count):
        keep = jnp.logical_or(position >= TXT, position < count)
        key_bias = jnp.where(keep, 0.0, MASKED).astype(jnp.bfloat16)
        query, keys, values = projections(states, is_text, modulation, w_qkv, q_gain, k_gain)
        key_heads = keys.astype(jnp.float32).reshape(TOKENS, HEADS, HEAD)
        value_heads = values.astype(jnp.float32).reshape(TOKENS, HEADS, HEAD)
        bias_wide = key_bias.astype(jnp.float32)
        query_blocks = query.reshape(TOKENS // query_rows, query_rows, HEADS * HEAD)

        def attend(block):
            return attend_block(block, key_heads, value_heads, bias_wide)
        attended = lax.map(attend, query_blocks).reshape(TOKENS, HEADS * HEAD)
        return gate * jnp.dot(attended, w_out, preferred_element_type=jnp.float32)
    cond = one_branch(hidden[0], text_count[0])
    uncond = one_branch(hidden[1], text_count[1])
    return uncond + GUIDANCE * (cond - uncond)
```

```python
import functools

import jax
import jax.numpy as jnp
from jax import lax
from jax.experimental import pallas as pl
from jax.experimental.pallas import tpu as pltpu
from jax.sharding import PartitionSpec as P

HEAD = 64
HEADS = 16
TXT = 226


GUIDANCE = 6.0
EPSILON = 1e-05
MASKED = -1000000000.0


def swapped(block, axis, apart):
    count = lax.axis_size(axis)
    route = []
    for low in range(count):
        high = low | 1 << apart
        if high != low and high < count:
            route += [(low, high), (high, low)]
    return lax.ppermute(block, axis, route)


def layer_normal(values_in):
    average = jnp.mean(values_in, axis=-1, keepdims=True)
    centred = values_in - average
    spread = jnp.mean(centred * centred, axis=-1, keepdims=True)
    return centred * lax.rsqrt(spread + EPSILON)


def modulated(states, is_text, modulation):
    normed = layer_normal(states.astype(jnp.float32))
    shift = jnp.where(is_text[:, None], modulation[3][None, :], modulation[0][None, :])
    scale = jnp.where(is_text[:, None], modulation[4][None, :], modulation[1][None, :])
    return (normed * (1.0 + scale) + shift).astype(jnp.bfloat16)


def head_normal(projected, gain):
    rows = projected.shape[0]
    heads_view = projected.reshape(rows, HEADS, HEAD)
    return (layer_normal(heads_view) * gain).reshape(rows, HEADS * HEAD).astype(jnp.bfloat16)


def projections(states, is_text, modulation, w_qkv, q_gain, k_gain):
    modded = modulated(states, is_text, modulation)
    query = head_normal(jnp.dot(modded, w_qkv[0], preferred_element_type=jnp.float32), q_gain)
    keys = head_normal(jnp.dot(modded, w_qkv[1], preferred_element_type=jnp.float32), k_gain)
    values = jnp.dot(modded, w_qkv[2], preferred_element_type=jnp.float32).astype(jnp.bfloat16)
    return (query, keys, values)


def fold_block(query_heads, carry, piece):
    highest, total, numer = carry
    keys_piece, values_piece, bias_piece = piece
    count = keys_piece.shape[0]
    key_heads = keys_piece.reshape(count, HEADS, HEAD)
    value_heads = values_piece.reshape(count, HEADS, HEAD)
    scores = jnp.einsum("qhd,khd->hqk", query_heads, key_heads, preferred_element_type=jnp.float32)
    scores = scores * HEAD ** (-0.5) + bias_piece.astype(jnp.float32)[None, None, :]
    new_high = jnp.maximum(highest, jnp.max(scores, axis=-1))
    expo = jnp.exp(scores - new_high[:, :, None])
    rescale = jnp.exp(highest - new_high)
    total = jnp.sum(expo, axis=-1)
    numer = numer * rescale.T[:, :, None] + jnp.einsum(
        "hqk,khd->qhd", expo.astype(jnp.bfloat16), value_heads, preferred_element_type=jnp.float32
    )
    return (new_high, total, numer)


def shards(hidden, modulation, w_qkv, q_gain, k_gain, w_out, text_count, block_order):
    states = hidden[0]
    tok_rows = states.shape[0]
    within = jnp.arange(tok_rows, dtype=jnp.int32)
    position = block_order[0] * tok_rows + within
    is_text = position < TXT
    keep = jnp.logical_or(position >= TXT, position < text_count[0])
    key_bias = jnp.where(keep, 0.0, MASKED).astype(jnp.bfloat16)
    query, keys, values = projections(states, is_text, modulation, w_qkv, q_gain, k_gain)
    query_heads = query.reshape(tok_rows, HEADS, HEAD)
    start_state = (
        jnp.full((HEADS, tok_rows), -1e30, jnp.float32),
        jnp.zeros((HEADS, tok_rows), jnp.float32),
        jnp.zeros((tok_rows, HEADS, HEAD), jnp.float32),
    )
    carry = fold_block(
        query_heads,
        start_state,
        (
            lax.all_gather(keys, "seq", axis=0, tiled=True),
            lax.all_gather(values, "seq", axis=0, tiled=True),
            lax.all_gather(key_bias, "seq", axis=0, tiled=True),
        ),
    )
    highest, total, numer = carry
    attended = (numer / total.T[:, :, None]).reshape(tok_rows, HEADS * HEAD).astype(jnp.bfloat16)
    gate = jnp.where(is_text[:, None], modulation[5][None, :], modulation[2][None, :])
    cfg_index = lax.axis_index("cfg")
    half_width = w_out.shape[1] // 2
    w_half = lax.dynamic_slice_in_dim(w_out, cfg_index * half_width, half_width, 1)
    gate_half = lax.dynamic_slice_in_dim(gate, cfg_index * half_width, half_width, 1)
    partner = swapped(attended, "cfg", 0)
    own_update = gate_half * jnp.dot(attended, w_half, preferred_element_type=jnp.float32)
    other_update = gate_half * jnp.dot(partner, w_half, preferred_element_type=jnp.float32)
    is_first = cfg_index == 0
    cond = jnp.where(is_first, own_update, other_update)
    uncond = jnp.where(is_first, other_update, own_update)
    return uncond + GUIDANCE * (cond - uncond)


LANES = 128
GROUPS = 4
MESH = pl.DeviceIdType.MESH


def flip(bit, other):
    return lax.rem(bit + other, 2)


def column_normal(x):
    centred = x - jnp.mean(x, axis=0, keepdims=True)
    spread = jnp.mean(centred * centred, axis=0, keepdims=True)
    return centred * lax.rsqrt(spread + EPSILON)


def fused(n, count_ref, block_ref, hidden_ref, mod_ref, w_ref, qg_ref, kg_ref, wo_ref, out_ref,
          count_v, block_v, hidden_v, mod_v, qg_v, kg_v, w_buf, wo_buf, wo_turned, gate, modded,
          kv_out, kv_in, q_out, q_in, place_out, place_in, keys, values,
          att_own, att_far, mixed, att_in,
          in_sem, w_sem, wo_sem, kv_s, kv_r, q_s, q_r, p_s, p_r, x_s, x_r, a_s, a_r):
    me = lax.axis_index("seq")
    cfg = lax.axis_index("cfg")
    rows, width = hidden_ref.shape
    half = width // 2
    wide = wo_buf.shape[1]
    excess = wide - half
    cols = w_buf.shape[3]
    heads_here = cols // HEAD
    steps = n // 2
    span = n * rows // 2
    bf, f32 = jnp.bfloat16, jnp.float32
    plane = lax.div(me, GROUPS)
    plane_high, plane_low = lax.div(plane, 2), lax.rem(plane, 2)
    side, core = lax.rem(lax.div(me, 2), 2), lax.rem(me, 2)

    barrier = pltpu.get_barrier_semaphore()
    for j in range(1, n):
        pl.semaphore_signal(barrier, inc=1, device_id={"seq": lax.rem(me + j, n)}, device_id_type=MESH)
    pl.semaphore_signal(barrier, inc=1, device_id={"cfg": 1 - cfg}, device_id_type=MESH)

    def group(i):
        high = 1 - lax.div(i, 2)
        lowbit = flip(lax.div(i, 2), lax.rem(i, 2))
        return 2 * flip(plane_high, high) + flip(plane_low, lowbit)

    def member(first, h):
        return first + 2 * flip(side, h // 2) + flip(core, h % 2)

    def weight(kind, i):
        start = pl.multiple_of(group(i) * cols, cols)
        return pltpu.make_async_copy(
            w_ref.at[kind, :, pl.ds(start, cols)], w_buf.at[kind, i], w_sem.at[kind, i])

    column = pl.multiple_of(cfg * (width - wide), LANES)
    out_weight = pltpu.make_async_copy(wo_ref.at[:, pl.ds(column, wide)], wo_buf, wo_sem)
    inputs = [pltpu.make_async_copy(a, b, in_sem.at[i]) for i, (a, b) in enumerate([
        (hidden_ref, hidden_v), (mod_ref, mod_v), (block_ref, block_v), (count_ref, count_v),
        (kg_ref, kg_v), (qg_ref, qg_v)])]
    for copy in inputs:
        copy.start()
    weight(1, 0).start()
    weight(2, 0).start()

    def send(src, dst, to, s_sem, r_sem):
        @pl.when(to != me)
        def _():
            pltpu.make_async_remote_copy(
                src_ref=src.at[to], dst_ref=dst.at[me], send_sem=s_sem, recv_sem=r_sem,
                device_id={"seq": to}, device_id_type=MESH).start()

        @pl.when(to == me)
        def _():
            dst[me] = src[to]

    def landed(ref, count, sem):
        part = ref.at[pl.ds(0, count)]
        pltpu.make_async_copy(part, part, sem).wait()

    for copy in inputs:
        copy.wait()
    block = block_v[...]
    count = count_v[...]
    mod = mod_v[...]
    down = block * rows + lax.broadcasted_iota(jnp.int32, (rows, 1), 0)
    is_text = down < TXT
    normed = layer_normal(hidden_v[...].astype(f32))
    shift = jnp.where(is_text, mod[3:4, :], mod[0:1, :])
    scale = jnp.where(is_text, mod[4:5, :], mod[1:2, :])
    modded[...] = (normed * (1.0 + scale) + shift).astype(bf)

    for i in range(1, GROUPS):
        weight(1, i).start()
        weight(2, i).start()
    for i in range(GROUPS):
        weight(0, i).start()
    out_weight.start()

    def down_lanes(gain_row):
        both = jnp.concatenate([gain_row, gain_row], axis=1)
        return jnp.broadcast_to(both, (LANES, LANES)).T[:HEAD]

    k_gain = down_lanes(kg_v[...])
    q_gain = down_lanes(qg_v[...]) * HEAD ** (-0.5)
    place_out[0] = jnp.broadcast_to(block, (1, LANES))
    place_in[me] = jnp.broadcast_to(block, (1, LANES))

    def project_kv(i):
        weight(1, i).wait()
        weight(2, i).wait()
        first = group(i) * heads_here
        x = modded[...]
        k_all = jnp.dot(x, w_buf[1, i], preferred_element_type=f32).T
        v_all = jnp.dot(x, w_buf[2, i], preferred_element_type=f32).T
        for h in range(heads_here):
            part = slice(h * HEAD, (h + 1) * HEAD)
            kv_out[first + h, :HEAD] = (column_normal(k_all[part]) * k_gain).astype(bf)
            kv_out[first + h, HEAD:] = v_all[part].astype(bf)

    def send_kv(i):
        first = group(i) * heads_here
        for h in range(heads_here):
            send(kv_out, kv_in, member(first, h), kv_s, kv_r)

    project_kv(0)
    pl.semaphore_wait(barrier, n)
    send_kv(0)
    for j in range(1, n):
        pltpu.make_async_remote_copy(
            src_ref=place_out.at[0], dst_ref=place_in.at[me], send_sem=p_s, recv_sem=p_r,
            device_id={"seq": lax.rem(me + j, n)}, device_id_type=MESH).start()

    def rest_kv(i, carry):
        project_kv(i)
        send_kv(i)
        return carry

    lax.fori_loop(1, GROUPS, rest_kv, 0)

    def project_q(i, carry):
        weight(0, i).wait()
        first = group(i) * heads_here
        q_all = jnp.dot(modded[...], w_buf[0, i], preferred_element_type=f32).T
        for h in range(heads_here):
            part = slice(h * HEAD, (h + 1) * HEAD)
            q_out[first + h] = (column_normal(q_all[part]) * q_gain).astype(bf)
        for h in range(heads_here):
            send(q_out, q_in, member(first, h), q_s, q_r.at[me])
        return carry

    lax.fori_loop(0, GROUPS, project_q, 0)

    out_weight.wait()

    def put(target, turned, c):
        @pl.when(cfg == 0)
        def _():
            low, high = c * LANES, min((c + 1) * LANES, half)
            target[low:high] = turned[:high - low]

        @pl.when(cfg != 0)
        def _():
            low, high = max(c * LANES - excess, 0), (c + 1) * LANES - excess
            target[low:high] = turned[LANES - (high - low):]

    gate_text = jnp.where(cfg == 0, mod_v[5:6, :wide], mod_v[5:6, width - wide:])
    gate_video = jnp.where(cfg == 0, mod_v[2:3, :wide], mod_v[2:3, width - wide:])
    for c in range(wide // LANES):
        part = slice(c * LANES, (c + 1) * LANES)
        put(gate, jnp.where(is_text, gate_text[:, part], gate_video[:, part]).T, c)
        for g in range(GROUPS):
            put(wo_turned.at[g], wo_buf[g * cols:(g + 1) * cols, part].T, c)

    landed(place_in, n - 1, p_r)
    lane = lax.broadcasted_iota(jnp.int32, (rows, LANES), 1)
    sub = lax.broadcasted_iota(jnp.int32, (rows, LANES), 0)

    def masked(j):
        at = place_in[j] * rows + sub
        return jnp.where(jnp.logical_or(at >= TXT, at < count), 0.0, MASKED)

    for p in range(steps):
        even, odd = masked(2 * p), masked(2 * p + 1)
        keys[p * rows:(p + 1) * rows, LANES:] = jnp.where(
            lane == 0, even, jnp.where(lane == 1, odd, 0.0)).astype(bf)
    values[HEAD:] = jnp.ones((values.shape[0] - HEAD, n * rows), bf)

    landed(kv_in, n - 1, kv_r)
    for p in range(steps):
        both = jnp.concatenate([kv_in[2 * p, :HEAD], kv_in[2 * p + 1, :HEAD]], axis=0)
        keys[p * rows:(p + 1) * rows, :LANES] = both.T
        values[:HEAD, p * rows:(p + 1) * rows] = kv_in[2 * p, HEAD:]
        values[:HEAD, span + p * rows:span + (p + 1) * rows] = kv_in[2 * p + 1, HEAD:]

    chip = lax.div(me, 2)

    def chip_of(k):
        mask = jnp.where(k == 0, 1, jnp.where(k <= 4, k + 3, jnp.where(k <= 6, k - 3, 0)))
        c0, c1, c2 = lax.rem(chip, 2), lax.rem(lax.div(chip, 2), 2), lax.div(chip, 4)
        k0, k1, k2 = lax.rem(mask, 2), lax.rem(lax.div(mask, 2), 2), lax.div(mask, 4)
        return 4 * flip(c2, k2) + 2 * flip(c1, k1) + flip(c0, k0)

    own_weight = jnp.where(cfg == 0, GUIDANCE, 1.0 - GUIDANCE)
    far_weight = 1.0 - own_weight

    def give(k):
        pair = chip_of(k)
        base = 2 * pair
        part = att_far.at[pl.ds(base, 2)]
        pltpu.make_async_copy(part, part, x_r.at[pair]).wait()
        for i in range(2):
            blend = own_weight * att_own[base + i].astype(f32) + far_weight * att_far[base + i].astype(f32)
            mixed[base + i] = blend.astype(bf)
            send(mixed, att_in, base + i, a_s, a_r.at[plane])

    row = lax.broadcasted_iota(jnp.int32, (LANES, 2 * rows), 0)
    first_row = jnp.where(row == 0, 1.0, 0.0).astype(bf)
    second_row = jnp.where(row == 1, 1.0, 0.0).astype(bf)
    blank = jnp.zeros((HEAD, 2 * rows), bf)

    def attend(k, carry):
        pair = chip_of(k)
        base = 2 * pair
        for i in range(2):
            @pl.when(base + i != me)
            def _():
                pltpu.make_async_copy(q_in.at[base + i], q_in.at[base + i], q_r.at[base + i]).wait()
        query = jnp.concatenate([q_in[base], q_in[base + 1]], axis=1)
        upper = jnp.concatenate([query, blank, first_row], axis=0)
        lower = jnp.concatenate([blank, query, second_row], axis=0)
        even = jnp.dot(keys[...], upper, preferred_element_type=f32)
        odd = jnp.dot(keys[...], lower, preferred_element_type=f32)
        highest = jnp.maximum(jnp.max(even, axis=0, keepdims=True), jnp.max(odd, axis=0, keepdims=True))
        numer = jnp.dot(values[:, :span], jnp.exp(even - highest).astype(bf), preferred_element_type=f32)
        numer += jnp.dot(values[:, span:], jnp.exp(odd - highest).astype(bf), preferred_element_type=f32)
        result = (numer[:HEAD] / numer[HEAD:HEAD + 1]).astype(bf)
        att_own[base] = result[:, :rows]
        att_own[base + 1] = result[:, rows:]
        pltpu.make_async_remote_copy(
            src_ref=att_own.at[pl.ds(base, 2)], dst_ref=att_far.at[pl.ds(base, 2)],
            send_sem=x_s, recv_sem=x_r.at[pair],
            device_id={"cfg": 1 - cfg}, device_id_type=MESH).start()

        @pl.when(k >= 2)
        def _():
            give(k - 2)

        return carry

    lax.fori_loop(0, steps, attend, 0)
    give(steps - 2)
    give(steps - 1)

    total = None
    for i in (3, 2, 0, 1):
        g = group(i)
        landed(att_in, heads_here - 1 if i == 3 else heads_here, a_r.at[g])
        part = att_in[pl.ds(g * heads_here, heads_here)].reshape(cols, rows)
        term = jnp.dot(wo_turned[g], part, preferred_element_type=f32)
        total = term if total is None else total + term
    out_ref[...] = gate[...] * total

    landed(kv_out, n - 1, kv_s)
    landed(q_out, n - 1, q_s)
    landed(place_in, n - 1, p_s)
    landed(att_own, n, x_s)
    landed(mixed, n - 1, a_s)


def whole_kernel(hidden, modulation, w_qkv, q_gain, k_gain, w_out, text_count, block_order):
    n = lax.axis_size("seq")
    states = hidden[0]
    rows, width = states.shape
    features = w_out.shape[0]
    cols = features // GROUPS
    half = width // 2
    wide = -(-half // LANES) * LANES
    bf, f32 = jnp.bfloat16, jnp.float32
    hbm = pl.BlockSpec(memory_space=pltpu.HBM)
    dma = pltpu.SemaphoreType.DMA
    turned = pl.pallas_call(
        functools.partial(fused, n),
        out_shape=jax.ShapeDtypeStruct((half, rows), f32),
        in_specs=[hbm] * 8,
        out_specs=pl.BlockSpec(memory_space=pltpu.VMEM),
        scratch_shapes=[
            pltpu.VMEM((1, 1), jnp.int32),
            pltpu.VMEM((1, 1), jnp.int32),
            pltpu.VMEM((rows, width), bf),
            pltpu.VMEM(modulation.shape, f32),
            pltpu.VMEM((1, HEAD), f32),
            pltpu.VMEM((1, HEAD), f32),
            pltpu.VMEM((3, GROUPS, width, cols), bf),
            pltpu.VMEM((features, wide), bf),
            pltpu.VMEM((GROUPS, half, cols), bf),
            pltpu.VMEM((half, rows), f32),
            pltpu.VMEM((rows, width), bf),
            pltpu.VMEM((n, 2 * HEAD, rows), bf),
            pltpu.VMEM((n, 2 * HEAD, rows), bf),
            pltpu.VMEM((n, HEAD, rows), bf),
            pltpu.VMEM((n, HEAD, rows), bf),
            pltpu.VMEM((1, 1, LANES), jnp.int32),
            pltpu.VMEM((n, 1, LANES), jnp.int32),
            pltpu.VMEM((n * rows // 2, 2 * LANES), bf),
            pltpu.VMEM((HEAD + 16, n * rows), bf),
        ] + [pltpu.VMEM((n, HEAD, rows), bf)] * 4 + [
            dma((6,)), dma((3, GROUPS)), dma,
            dma, dma, dma, dma((n,)), dma, dma, dma, dma((n // 2,)), dma, dma((GROUPS,)),
        ],
        compiler_params=pltpu.CompilerParams(
            collective_id=0, has_side_effects=True, vmem_limit_bytes=40 * 1024 * 1024),
    )(text_count[None], block_order[None], states, modulation, w_qkv, q_gain[None], k_gain[None], w_out)
    return turned.T


def solution(mesh):
    in_specs = (P("cfg", "seq", None), P(), P(), P(), P(), P(), P("cfg"), P("seq"))
    out_specs = P("seq", "cfg")
    one_head_each = mesh.shape["seq"] == HEADS and mesh.shape["cfg"] == 2
    body = whole_kernel if one_head_each else shards
    return jax.shard_map(body, mesh=mesh, in_specs=in_specs, out_specs=out_specs, check_vma=False)
```

```python
import functools

import jax
import jax.numpy as jnp
from jax import lax
from jax.experimental import pallas as pl
from jax.experimental.pallas import tpu as pltpu
from jax.sharding import PartitionSpec as P

HEAD = 64
HEADS = 16
TXT = 226


GUIDANCE = 6.0
EPSILON = 1e-05
MASKED = -1000000000.0


def swapped(block, axis, apart):
    count = lax.axis_size(axis)
    route = []
    for low in range(count):
        high = low | 1 << apart
        if high != low and high < count:
            route += [(low, high), (high, low)]
    return lax.ppermute(block, axis, route)


def layer_normal(values_in):
    average = jnp.mean(values_in, axis=-1, keepdims=True)
    centred = values_in - average
    spread = jnp.mean(centred * centred, axis=-1, keepdims=True)
    return centred * lax.rsqrt(spread + EPSILON)


def modulated(states, is_text, modulation):
    normed = layer_normal(states.astype(jnp.float32))
    shift = jnp.where(is_text[:, None], modulation[3][None, :], modulation[0][None, :])
    scale = jnp.where(is_text[:, None], modulation[4][None, :], modulation[1][None, :])
    return (normed * (1.0 + scale) + shift).astype(jnp.bfloat16)


def head_normal(projected, gain):
    rows = projected.shape[0]
    heads_view = projected.reshape(rows, HEADS, HEAD)
    return (layer_normal(heads_view) * gain).reshape(rows, HEADS * HEAD).astype(jnp.bfloat16)


def projections(states, is_text, modulation, w_qkv, q_gain, k_gain):
    modded = modulated(states, is_text, modulation)
    query = head_normal(jnp.dot(modded, w_qkv[0], preferred_element_type=jnp.float32), q_gain)
    keys = head_normal(jnp.dot(modded, w_qkv[1], preferred_element_type=jnp.float32), k_gain)
    values = jnp.dot(modded, w_qkv[2], preferred_element_type=jnp.float32).astype(jnp.bfloat16)
    return (query, keys, values)


def fold_block(query_heads, carry, piece):
    highest, total, numer = carry
    keys_piece, values_piece, bias_piece = piece
    count = keys_piece.shape[0]
    key_heads = keys_piece.reshape(count, HEADS, HEAD)
    value_heads = values_piece.reshape(count, HEADS, HEAD)
    scores = jnp.einsum("qhd,khd->hqk", query_heads, key_heads, preferred_element_type=jnp.float32)
    scores = scores * HEAD ** (-0.5) + bias_piece.astype(jnp.float32)[None, None, :]
    new_high = jnp.maximum(highest, jnp.max(scores, axis=-1))
    expo = jnp.exp(scores - new_high[:, :, None])
    rescale = jnp.exp(highest - new_high)
    total = jnp.sum(expo, axis=-1)
    numer = numer * rescale.T[:, :, None] + jnp.einsum(
        "hqk,khd->qhd", expo.astype(jnp.bfloat16), value_heads, preferred_element_type=jnp.float32
    )
    return (new_high, total, numer)


def shards(hidden, modulation, w_qkv, q_gain, k_gain, w_out, text_count, block_order):
    states = hidden[0]
    tok_rows = states.shape[0]
    within = jnp.arange(tok_rows, dtype=jnp.int32)
    position = block_order[0] * tok_rows + within
    is_text = position < TXT
    keep = jnp.logical_or(position >= TXT, position < text_count[0])
    key_bias = jnp.where(keep, 0.0, MASKED).astype(jnp.bfloat16)
    query, keys, values = projections(states, is_text, modulation, w_qkv, q_gain, k_gain)
    query_heads = query.reshape(tok_rows, HEADS, HEAD)
    start_state = (
        jnp.full((HEADS, tok_rows), -1e30, jnp.float32),
        jnp.zeros((HEADS, tok_rows), jnp.float32),
        jnp.zeros((tok_rows, HEADS, HEAD), jnp.float32),
    )
    carry = fold_block(
        query_heads,
        start_state,
        (
            lax.all_gather(keys, "seq", axis=0, tiled=True),
            lax.all_gather(values, "seq", axis=0, tiled=True),
            lax.all_gather(key_bias, "seq", axis=0, tiled=True),
        ),
    )
    highest, total, numer = carry
    attended = (numer / total.T[:, :, None]).reshape(tok_rows, HEADS * HEAD).astype(jnp.bfloat16)
    gate = jnp.where(is_text[:, None], modulation[5][None, :], modulation[2][None, :])
    cfg_index = lax.axis_index("cfg")
    half_width = w_out.shape[1] // 2
    w_half = lax.dynamic_slice_in_dim(w_out, cfg_index * half_width, half_width, 1)
    gate_half = lax.dynamic_slice_in_dim(gate, cfg_index * half_width, half_width, 1)
    partner = swapped(attended, "cfg", 0)
    own_update = gate_half * jnp.dot(attended, w_half, preferred_element_type=jnp.float32)
    other_update = gate_half * jnp.dot(partner, w_half, preferred_element_type=jnp.float32)
    is_first = cfg_index == 0
    cond = jnp.where(is_first, own_update, other_update)
    uncond = jnp.where(is_first, other_update, own_update)
    return uncond + GUIDANCE * (cond - uncond)


LANES = 128
GROUPS = 4
SHIFT = 256
MESH = pl.DeviceIdType.MESH


def flip(bit, other):
    return lax.rem(bit + other, 2)


def column_normal(x):
    centred = x - jnp.mean(x, axis=0, keepdims=True)
    spread = jnp.mean(centred * centred, axis=0, keepdims=True)
    return centred * lax.rsqrt(spread + EPSILON)


def fused(n, info_ref, hidden_ref, mod_ref, w_ref, qg_ref, kg_ref, wo_ref, out_ref,
          hidden_v, mod_v, qg_v, kg_v, w_buf, wo_buf, wo_turned, gate, modded,
          kv_out, kv_in, q_out, q_in, place_out, place_in, keys, values,
          att_own, att_far, mixed, att_in,
          in_sem, w_sem, wo_sem, kv_s, kv_r, q_s, q_r, p_s, p_r, x_s, x_r, a_s, a_r):
    me = lax.axis_index("seq")
    cfg = lax.axis_index("cfg")
    rows, width = hidden_ref.shape
    half = width // 2
    wide = wo_buf.shape[1]
    excess = wide - half
    cols = w_buf.shape[3]
    heads_here = cols // HEAD
    steps = n // 2
    span = n * rows // 2
    bf, f32 = jnp.bfloat16, jnp.float32
    plane = lax.div(me, GROUPS)
    plane_high, plane_low = lax.div(plane, 2), lax.rem(plane, 2)
    side, core = lax.rem(lax.div(me, 2), 2), lax.rem(me, 2)

    barrier = pltpu.get_barrier_semaphore()
    for j in range(1, n):
        pl.semaphore_signal(barrier, inc=1, device_id={"seq": lax.rem(me + j, n)}, device_id_type=MESH)
    pl.semaphore_signal(barrier, inc=1, device_id={"cfg": 1 - cfg}, device_id_type=MESH)

    def group(i):
        high = 1 - lax.div(i, 2)
        lowbit = flip(lax.div(i, 2), lax.rem(i, 2))
        return 2 * flip(plane_high, high) + flip(plane_low, lowbit)

    def member(first, h):
        return first + 2 * flip(side, h // 2) + flip(core, h % 2)

    def weight(kind, i):
        start = pl.multiple_of(group(i) * cols, cols)
        return pltpu.make_async_copy(
            w_ref.at[kind, :, pl.ds(start, cols)], w_buf.at[kind, i], w_sem.at[kind, i])

    column = pl.multiple_of(cfg * (width - wide), LANES)
    out_weight = pltpu.make_async_copy(wo_ref.at[:, pl.ds(column, wide)], wo_buf, wo_sem)
    inputs = [pltpu.make_async_copy(a, b, in_sem.at[i]) for i, (a, b) in enumerate([
        (hidden_ref, hidden_v), (mod_ref, mod_v),
        (kg_ref, kg_v), (qg_ref, qg_v)])]
    for copy in inputs:
        copy.start()
    weight(1, 0).start()
    weight(2, 0).start()

    def send(src, dst, to, s_sem, r_sem):
        @pl.when(to != me)
        def _():
            pltpu.make_async_remote_copy(
                src_ref=src.at[to], dst_ref=dst.at[me], send_sem=s_sem, recv_sem=r_sem,
                device_id={"seq": to}, device_id_type=MESH).start()

        @pl.when(to == me)
        def _():
            dst[me] = src[to]

    def landed(ref, count, sem):
        part = ref.at[pl.ds(0, count)]
        pltpu.make_async_copy(part, part, sem).wait()

    for copy in inputs:
        copy.wait()
    block = lax.div(info_ref[0], SHIFT)
    count = lax.rem(info_ref[0], SHIFT)
    mod = mod_v[...]
    down = block * rows + lax.broadcasted_iota(jnp.int32, (rows, 1), 0)
    is_text = down < TXT
    normed = layer_normal(hidden_v[...].astype(f32))
    shift = jnp.where(is_text, mod[3:4, :], mod[0:1, :])
    scale = jnp.where(is_text, mod[4:5, :], mod[1:2, :])
    modded[...] = (normed * (1.0 + scale) + shift).astype(bf)

    for i in range(1, GROUPS):
        weight(1, i).start()
        weight(2, i).start()
    for i in range(GROUPS):
        weight(0, i).start()
    out_weight.start()

    def down_lanes(gain_row):
        both = jnp.concatenate([gain_row, gain_row], axis=1)
        return jnp.broadcast_to(both, (LANES, LANES)).T[:HEAD]

    k_gain = down_lanes(kg_v[...])
    q_gain = down_lanes(qg_v[...]) * HEAD ** (-0.5)
    place_out[0] = jnp.full((1, LANES), block, jnp.int32)
    place_in[me] = jnp.full((1, LANES), block, jnp.int32)

    def project_kv(i):
        weight(1, i).wait()
        weight(2, i).wait()
        first = group(i) * heads_here
        x = modded[...]
        k_all = jnp.dot(x, w_buf[1, i], preferred_element_type=f32).T
        v_all = jnp.dot(x, w_buf[2, i], preferred_element_type=f32).T
        for h in range(heads_here):
            part = slice(h * HEAD, (h + 1) * HEAD)
            kv_out[first + h, :HEAD] = (column_normal(k_all[part]) * k_gain).astype(bf)
            kv_out[first + h, HEAD:] = v_all[part].astype(bf)

    def send_kv(i):
        first = group(i) * heads_here
        for h in range(heads_here):
            send(kv_out, kv_in, member(first, h), kv_s, kv_r)

    project_kv(0)
    pl.semaphore_wait(barrier, n)
    send_kv(0)
    for j in range(1, n):
        pltpu.make_async_remote_copy(
            src_ref=place_out.at[0], dst_ref=place_in.at[me], send_sem=p_s, recv_sem=p_r,
            device_id={"seq": lax.rem(me + j, n)}, device_id_type=MESH).start()

    def rest_kv(i, carry):
        project_kv(i)
        send_kv(i)
        return carry

    lax.fori_loop(1, GROUPS, rest_kv, 0)

    def project_q(i, carry):
        weight(0, i).wait()
        first = group(i) * heads_here
        q_all = jnp.dot(modded[...], w_buf[0, i], preferred_element_type=f32).T
        for h in range(heads_here):
            part = slice(h * HEAD, (h + 1) * HEAD)
            q_out[first + h] = (column_normal(q_all[part]) * q_gain).astype(bf)
        for h in range(heads_here):
            send(q_out, q_in, member(first, h), q_s, q_r.at[me])
        return carry

    lax.fori_loop(0, GROUPS, project_q, 0)

    out_weight.wait()

    def put(target, turned, c):
        @pl.when(cfg == 0)
        def _():
            low, high = c * LANES, min((c + 1) * LANES, half)
            target[low:high] = turned[:high - low]

        @pl.when(cfg != 0)
        def _():
            low, high = max(c * LANES - excess, 0), (c + 1) * LANES - excess
            target[low:high] = turned[LANES - (high - low):]

    gate_text = jnp.where(cfg == 0, mod_v[5:6, :wide], mod_v[5:6, width - wide:])
    gate_video = jnp.where(cfg == 0, mod_v[2:3, :wide], mod_v[2:3, width - wide:])
    for c in range(wide // LANES):
        part = slice(c * LANES, (c + 1) * LANES)
        put(gate, jnp.where(is_text, gate_text[:, part], gate_video[:, part]).T, c)
        for g in range(GROUPS):
            put(wo_turned.at[g], wo_buf[g * cols:(g + 1) * cols, part].T, c)

    landed(place_in, n - 1, p_r)
    lane = lax.broadcasted_iota(jnp.int32, (rows, LANES), 1)
    sub = lax.broadcasted_iota(jnp.int32, (rows, LANES), 0)

    def masked(j):
        at = place_in[j] * rows + sub
        return jnp.where(jnp.logical_or(at >= TXT, at < count), 0.0, MASKED)

    for p in range(steps):
        even, odd = masked(2 * p), masked(2 * p + 1)
        keys[p * rows:(p + 1) * rows, LANES:] = jnp.where(
            lane == 0, even, jnp.where(lane == 1, odd, 0.0)).astype(bf)
    values[HEAD:] = jnp.ones((values.shape[0] - HEAD, n * rows), bf)

    landed(kv_in, n - 1, kv_r)
    for p in range(steps):
        both = jnp.concatenate([kv_in[2 * p, :HEAD], kv_in[2 * p + 1, :HEAD]], axis=0)
        keys[p * rows:(p + 1) * rows, :LANES] = both.T
        values[:HEAD, p * rows:(p + 1) * rows] = kv_in[2 * p, HEAD:]
        values[:HEAD, span + p * rows:span + (p + 1) * rows] = kv_in[2 * p + 1, HEAD:]

    chip = lax.div(me, 2)

    def chip_of(k):
        mask = jnp.where(k == 0, 1, jnp.where(k <= 4, k + 3, jnp.where(k <= 6, k - 3, 0)))
        c0, c1, c2 = lax.rem(chip, 2), lax.rem(lax.div(chip, 2), 2), lax.div(chip, 4)
        k0, k1, k2 = lax.rem(mask, 2), lax.rem(lax.div(mask, 2), 2), lax.div(mask, 4)
        return 4 * flip(c2, k2) + 2 * flip(c1, k1) + flip(c0, k0)

    own_weight = jnp.where(cfg == 0, GUIDANCE, 1.0 - GUIDANCE)
    far_weight = 1.0 - own_weight

    def give(k):
        pair = chip_of(k)
        base = 2 * pair
        part = att_far.at[pl.ds(base, 2)]
        pltpu.make_async_copy(part, part, x_r.at[pair]).wait()
        for i in range(2):
            blend = own_weight * att_own[base + i].astype(f32) + far_weight * att_far[base + i].astype(f32)
            mixed[base + i] = blend.astype(bf)
            send(mixed, att_in, base + i, a_s, a_r.at[plane])

    row = lax.broadcasted_iota(jnp.int32, (LANES, 2 * rows), 0)
    first_row = jnp.where(row == 0, 1.0, 0.0).astype(bf)
    second_row = jnp.where(row == 1, 1.0, 0.0).astype(bf)
    blank = jnp.zeros((HEAD, 2 * rows), bf)

    def attend(k, carry):
        pair = chip_of(k)
        base = 2 * pair
        for i in range(2):
            @pl.when(base + i != me)
            def _():
                pltpu.make_async_copy(q_in.at[base + i], q_in.at[base + i], q_r.at[base + i]).wait()
        query = jnp.concatenate([q_in[base], q_in[base + 1]], axis=1)
        upper = jnp.concatenate([query, blank, first_row], axis=0)
        lower = jnp.concatenate([blank, query, second_row], axis=0)
        even = jnp.dot(keys[...], upper, preferred_element_type=f32)
        odd = jnp.dot(keys[...], lower, preferred_element_type=f32)
        highest = jnp.maximum(jnp.max(even, axis=0, keepdims=True), jnp.max(odd, axis=0, keepdims=True))
        numer = jnp.dot(values[:, :span], jnp.exp(even - highest).astype(bf), preferred_element_type=f32)
        numer += jnp.dot(values[:, span:], jnp.exp(odd - highest).astype(bf), preferred_element_type=f32)
        result = (numer[:HEAD] / numer[HEAD:HEAD + 1]).astype(bf)
        att_own[base] = result[:, :rows]
        att_own[base + 1] = result[:, rows:]
        pltpu.make_async_remote_copy(
            src_ref=att_own.at[pl.ds(base, 2)], dst_ref=att_far.at[pl.ds(base, 2)],
            send_sem=x_s, recv_sem=x_r.at[pair],
            device_id={"cfg": 1 - cfg}, device_id_type=MESH).start()

        @pl.when(k >= 2)
        def _():
            give(k - 2)

        return carry

    lax.fori_loop(0, steps, attend, 0)
    give(steps - 2)
    give(steps - 1)

    total = None
    for i in (3, 2, 0, 1):
        g = group(i)
        landed(att_in, heads_here - 1 if i == 3 else heads_here, a_r.at[g])
        part = att_in[pl.ds(g * heads_here, heads_here)].reshape(cols, rows)
        term = jnp.dot(wo_turned[g], part, preferred_element_type=f32)
        total = term if total is None else total + term
    out_ref[...] = gate[...] * total

    landed(kv_out, n - 1, kv_s)
    landed(q_out, n - 1, q_s)
    landed(place_in, n - 1, p_s)
    landed(att_own, n, x_s)
    landed(mixed, n - 1, a_s)


def whole_kernel(hidden, modulation, w_qkv, q_gain, k_gain, w_out, text_count, block_order):
    n = lax.axis_size("seq")
    states = hidden[0]
    rows, width = states.shape
    features = w_out.shape[0]
    cols = features // GROUPS
    half = width // 2
    wide = -(-half // LANES) * LANES
    bf, f32 = jnp.bfloat16, jnp.float32
    hbm = pl.BlockSpec(memory_space=pltpu.HBM)
    dma = pltpu.SemaphoreType.DMA
    turned = pl.pallas_call(
        functools.partial(fused, n),
        out_shape=jax.ShapeDtypeStruct((half, rows), f32),
        in_specs=[pl.BlockSpec(memory_space=pltpu.SMEM)] + [hbm] * 6,
        out_specs=pl.BlockSpec(memory_space=pltpu.VMEM),
        scratch_shapes=[
            pltpu.VMEM((rows, width), bf),
            pltpu.VMEM(modulation.shape, f32),
            pltpu.VMEM((1, HEAD), f32),
            pltpu.VMEM((1, HEAD), f32),
            pltpu.VMEM((3, GROUPS, width, cols), bf),
            pltpu.VMEM((features, wide), bf),
            pltpu.VMEM((GROUPS, half, cols), bf),
            pltpu.VMEM((half, rows), f32),
            pltpu.VMEM((rows, width), bf),
            pltpu.VMEM((n, 2 * HEAD, rows), bf),
            pltpu.VMEM((n, 2 * HEAD, rows), bf),
            pltpu.VMEM((n, HEAD, rows), bf),
            pltpu.VMEM((n, HEAD, rows), bf),
            pltpu.VMEM((1, 1, LANES), jnp.int32),
            pltpu.VMEM((n, 1, LANES), jnp.int32),
            pltpu.VMEM((n * rows // 2, 2 * LANES), bf),
            pltpu.VMEM((HEAD + 16, n * rows), bf),
        ] + [pltpu.VMEM((n, HEAD, rows), bf)] * 4 + [
            dma((4,)), dma((3, GROUPS)), dma,
            dma, dma, dma, dma((n,)), dma, dma, dma, dma((n // 2,)), dma, dma((GROUPS,)),
        ],
        compiler_params=pltpu.CompilerParams(
            collective_id=0, has_side_effects=True, vmem_limit_bytes=40 * 1024 * 1024),
    )(block_order * SHIFT + text_count, *[pltpu.with_memory_space_constraint(x, pltpu.HBM) for x in (
        states, modulation, w_qkv, q_gain[None], k_gain[None], w_out)])
    return turned.T


def solution(mesh):
    in_specs = (P("cfg", "seq", None), P(), P(), P(), P(), P(), P("cfg"), P("seq"))
    out_specs = P("seq", "cfg")
    one_head_each = mesh.shape["seq"] == HEADS and mesh.shape["cfg"] == 2
    body = whole_kernel if one_head_each else shards
    return jax.shard_map(body, mesh=mesh, in_specs=in_specs, out_specs=out_specs, check_vma=False)
```

```python
import functools

import jax
import jax.numpy as jnp
from jax import lax
from jax.experimental import pallas as pl
from jax.experimental.pallas import tpu as pltpu
from jax.sharding import PartitionSpec as P

HEAD = 64
HEADS = 16
TXT = 226


GUIDANCE = 6.0
EPSILON = 1e-05
MASKED = -1000000000.0


def swapped(block, axis, apart):
    count = lax.axis_size(axis)
    route = []
    for low in range(count):
        high = low | 1 << apart
        if high != low and high < count:
            route += [(low, high), (high, low)]
    return lax.ppermute(block, axis, route)


def layer_normal(values_in):
    average = jnp.mean(values_in, axis=-1, keepdims=True)
    centred = values_in - average
    spread = jnp.mean(centred * centred, axis=-1, keepdims=True)
    return centred * lax.rsqrt(spread + EPSILON)


def modulated(states, is_text, modulation):
    normed = layer_normal(states.astype(jnp.float32))
    shift = jnp.where(is_text[:, None], modulation[3][None, :], modulation[0][None, :])
    scale = jnp.where(is_text[:, None], modulation[4][None, :], modulation[1][None, :])
    return (normed * (1.0 + scale) + shift).astype(jnp.bfloat16)


def head_normal(projected, gain):
    rows = projected.shape[0]
    heads_view = projected.reshape(rows, HEADS, HEAD)
    return (layer_normal(heads_view) * gain).reshape(rows, HEADS * HEAD).astype(jnp.bfloat16)


def projections(states, is_text, modulation, w_qkv, q_gain, k_gain):
    modded = modulated(states, is_text, modulation)
    query = head_normal(jnp.dot(modded, w_qkv[0], preferred_element_type=jnp.float32), q_gain)
    keys = head_normal(jnp.dot(modded, w_qkv[1], preferred_element_type=jnp.float32), k_gain)
    values = jnp.dot(modded, w_qkv[2], preferred_element_type=jnp.float32).astype(jnp.bfloat16)
    return (query, keys, values)


def fold_block(query_heads, carry, piece):
    highest, total, numer = carry
    keys_piece, values_piece, bias_piece = piece
    count = keys_piece.shape[0]
    key_heads = keys_piece.reshape(count, HEADS, HEAD)
    value_heads = values_piece.reshape(count, HEADS, HEAD)
    scores = jnp.einsum("qhd,khd->hqk", query_heads, key_heads, preferred_element_type=jnp.float32)
    scores = scores * HEAD ** (-0.5) + bias_piece.astype(jnp.float32)[None, None, :]
    new_high = jnp.maximum(highest, jnp.max(scores, axis=-1))
    expo = jnp.exp(scores - new_high[:, :, None])
    rescale = jnp.exp(highest - new_high)
    total = jnp.sum(expo, axis=-1)
    numer = numer * rescale.T[:, :, None] + jnp.einsum(
        "hqk,khd->qhd", expo.astype(jnp.bfloat16), value_heads, preferred_element_type=jnp.float32
    )
    return (new_high, total, numer)


def shards(hidden, modulation, w_qkv, q_gain, k_gain, w_out, text_count, block_order):
    states = hidden[0]
    tok_rows = states.shape[0]
    within = jnp.arange(tok_rows, dtype=jnp.int32)
    position = block_order[0] * tok_rows + within
    is_text = position < TXT
    keep = jnp.logical_or(position >= TXT, position < text_count[0])
    key_bias = jnp.where(keep, 0.0, MASKED).astype(jnp.bfloat16)
    query, keys, values = projections(states, is_text, modulation, w_qkv, q_gain, k_gain)
    query_heads = query.reshape(tok_rows, HEADS, HEAD)
    start_state = (
        jnp.full((HEADS, tok_rows), -1e30, jnp.float32),
        jnp.zeros((HEADS, tok_rows), jnp.float32),
        jnp.zeros((tok_rows, HEADS, HEAD), jnp.float32),
    )
    carry = fold_block(
        query_heads,
        start_state,
        (
            lax.all_gather(keys, "seq", axis=0, tiled=True),
            lax.all_gather(values, "seq", axis=0, tiled=True),
            lax.all_gather(key_bias, "seq", axis=0, tiled=True),
        ),
    )
    highest, total, numer = carry
    attended = (numer / total.T[:, :, None]).reshape(tok_rows, HEADS * HEAD).astype(jnp.bfloat16)
    gate = jnp.where(is_text[:, None], modulation[5][None, :], modulation[2][None, :])
    cfg_index = lax.axis_index("cfg")
    half_width = w_out.shape[1] // 2
    w_half = lax.dynamic_slice_in_dim(w_out, cfg_index * half_width, half_width, 1)
    gate_half = lax.dynamic_slice_in_dim(gate, cfg_index * half_width, half_width, 1)
    partner = swapped(attended, "cfg", 0)
    own_update = gate_half * jnp.dot(attended, w_half, preferred_element_type=jnp.float32)
    other_update = gate_half * jnp.dot(partner, w_half, preferred_element_type=jnp.float32)
    is_first = cfg_index == 0
    cond = jnp.where(is_first, own_update, other_update)
    uncond = jnp.where(is_first, other_update, own_update)
    return uncond + GUIDANCE * (cond - uncond)


LANES = 128
GROUPS = 4
SHIFT = 256
MESH = pl.DeviceIdType.MESH


def flip(bit, other):
    return lax.rem(bit + other, 2)


def column_normal(x):
    centred = x - jnp.mean(x, axis=0, keepdims=True)
    spread = jnp.mean(centred * centred, axis=0, keepdims=True)
    return centred * lax.rsqrt(spread + EPSILON)


def fused(n, info_ref, hidden_ref, mod_ref, w_ref, qg_ref, kg_ref, wo_ref, out_ref,
          hidden_v, mod_v, qg_v, kg_v, w_buf, wo_buf, wo_turned, gate, modded,
          kv_out, kv_in, q_out, q_in, place_out, place_in, keys, values,
          att_own, att_far, mixed, att_in, held_a, held_b,
          in_sem, w_sem, wo_sem, kv_s, kv_r, q_s, q_r, p_s, p_r, x_s, x_r, a_s, a_r):
    me = lax.axis_index("seq")
    cfg = lax.axis_index("cfg")
    rows, width = hidden_ref.shape
    half = width // 2
    wide = wo_buf.shape[1]
    excess = wide - half
    cols = w_buf.shape[3]
    heads_here = cols // HEAD
    steps = n // 2
    span = n * rows // 2
    bf, f32 = jnp.bfloat16, jnp.float32
    plane = lax.div(me, GROUPS)
    plane_high, plane_low = lax.div(plane, 2), lax.rem(plane, 2)
    side, core = lax.rem(lax.div(me, 2), 2), lax.rem(me, 2)

    barrier = pltpu.get_barrier_semaphore()
    for j in range(1, n):
        pl.semaphore_signal(barrier, inc=1, device_id={"seq": lax.rem(me + j, n)}, device_id_type=MESH)
    pl.semaphore_signal(barrier, inc=1, device_id={"cfg": 1 - cfg}, device_id_type=MESH)

    outer = plane_high == plane_low

    def group(i):
        mask = jnp.where(outer, lax.rem(i + 1, GROUPS), jnp.where(i == 3, 0, lax.rem(i + 1, 3) + 1))
        return 2 * flip(plane_high, lax.div(mask, 2)) + flip(plane_low, lax.rem(mask, 2))

    def member(first, h):
        return first + 2 * flip(side, h // 2) + flip(core, h % 2)

    def weight(kind, i):
        start = pl.multiple_of(group(i) * cols, cols)
        return pltpu.make_async_copy(
            w_ref.at[kind, :, pl.ds(start, cols)], w_buf.at[kind, i], w_sem.at[kind, i])

    column = pl.multiple_of(cfg * (width - wide), LANES)
    out_weight = pltpu.make_async_copy(wo_ref.at[:, pl.ds(column, wide)], wo_buf, wo_sem)
    inputs = [pltpu.make_async_copy(a, b, in_sem.at[i]) for i, (a, b) in enumerate([
        (hidden_ref, hidden_v), (mod_ref, mod_v),
        (kg_ref, kg_v), (qg_ref, qg_v)])]
    for copy in inputs:
        copy.start()
    weight(1, 0).start()
    weight(2, 0).start()

    def send(src, dst, to, s_sem, r_sem):
        @pl.when(to != me)
        def _():
            pltpu.make_async_remote_copy(
                src_ref=src.at[to], dst_ref=dst.at[me], send_sem=s_sem, recv_sem=r_sem,
                device_id={"seq": to}, device_id_type=MESH).start()

        @pl.when(to == me)
        def _():
            dst[me] = src[to]

    def landed(ref, count, sem):
        part = ref.at[pl.ds(0, count)]
        pltpu.make_async_copy(part, part, sem).wait()

    for copy in inputs:
        copy.wait()
    block = lax.div(info_ref[0], SHIFT)
    count = lax.rem(info_ref[0], SHIFT)
    mod = mod_v[...]
    down = block * rows + lax.broadcasted_iota(jnp.int32, (rows, 1), 0)
    is_text = down < TXT
    normed = layer_normal(hidden_v[...].astype(f32))
    shift = jnp.where(is_text, mod[3:4, :], mod[0:1, :])
    scale = jnp.where(is_text, mod[4:5, :], mod[1:2, :])
    modded[...] = (normed * (1.0 + scale) + shift).astype(bf)

    for i in range(1, GROUPS):
        weight(1, i).start()
        weight(2, i).start()
    for i in range(GROUPS):
        weight(0, i).start()
    out_weight.start()

    def down_lanes(gain_row):
        both = jnp.concatenate([gain_row, gain_row], axis=1)
        return jnp.broadcast_to(both, (LANES, LANES)).T[:HEAD]

    k_gain = down_lanes(kg_v[...])
    q_gain = down_lanes(qg_v[...]) * HEAD ** (-0.5)
    place_out[0] = jnp.full((1, LANES), block, jnp.int32)
    place_in[me] = jnp.full((1, LANES), block, jnp.int32)

    def project_kv(i):
        weight(1, i).wait()
        weight(2, i).wait()
        first = group(i) * heads_here
        x = modded[...]
        k_all = jnp.dot(x, w_buf[1, i], preferred_element_type=f32).T
        v_all = jnp.dot(x, w_buf[2, i], preferred_element_type=f32).T
        for h in range(heads_here):
            part = slice(h * HEAD, (h + 1) * HEAD)
            kv_out[first + h, :HEAD] = (column_normal(k_all[part]) * k_gain).astype(bf)
            kv_out[first + h, HEAD:] = v_all[part].astype(bf)

    def send_kv(i):
        if isinstance(i, int):
            pl.semaphore_wait(barrier, n)
            for j in range(1, n):
                pltpu.make_async_remote_copy(
                    src_ref=place_out.at[0], dst_ref=place_in.at[me], send_sem=p_s, recv_sem=p_r,
                    device_id={"seq": lax.rem(me + j, n)}, device_id_type=MESH).start()
        for h in range(heads_here):
            send(kv_out, kv_in, member(group(i) * heads_here, h), kv_s, kv_r)

    def rest_kv(i, carry):
        project_kv(i)
        send_kv(i)
        return carry

    project_kv(0)
    send_kv(0)
    lax.fori_loop(1, GROUPS, rest_kv, 0)

    def project_q(i):
        weight(0, i).wait()
        first = group(i) * heads_here
        q_all = jnp.dot(modded[...], w_buf[0, i], preferred_element_type=f32).T
        for h in range(heads_here):
            part = slice(h * HEAD, (h + 1) * HEAD)
            q_out[first + h] = (column_normal(q_all[part]) * q_gain).astype(bf)

    def send_q(i):
        for h in range(heads_here):
            send(q_out, q_in, member(group(i) * heads_here, h), q_s, q_r.at[me])

    lax.fori_loop(0, GROUPS, lambda i, carry: (project_q(i), carry)[1], 0)
    send_q(3)

    out_weight.wait()

    def put(target, turned, c):
        @pl.when(cfg == 0)
        def _():
            low, high = c * LANES, min((c + 1) * LANES, half)
            target[low:high] = turned[:high - low]

        @pl.when(cfg != 0)
        def _():
            low, high = max(c * LANES - excess, 0), (c + 1) * LANES - excess
            target[low:high] = turned[LANES - (high - low):]

    gate_text = jnp.where(cfg == 0, mod_v[5:6, :wide], mod_v[5:6, width - wide:])
    gate_video = jnp.where(cfg == 0, mod_v[2:3, :wide], mod_v[2:3, width - wide:])
    for c in range(wide // LANES):
        part = slice(c * LANES, (c + 1) * LANES)
        put(gate, jnp.where(is_text, gate_text[:, part], gate_video[:, part]).T, c)
        for g in range(GROUPS):
            put(wo_turned.at[g], wo_buf[g * cols:(g + 1) * cols, part].T, c)

    landed(place_in, n - 1, p_r)
    lane = lax.broadcasted_iota(jnp.int32, (rows, LANES), 1)
    sub = lax.broadcasted_iota(jnp.int32, (rows, LANES), 0)

    def masked(j):
        at = place_in[j] * rows + sub
        return jnp.where(jnp.logical_or(at >= TXT, at < count), 0.0, MASKED)

    for p in range(steps):
        even, odd = masked(2 * p), masked(2 * p + 1)
        keys[p * rows:(p + 1) * rows, LANES:] = jnp.where(
            lane == 0, even, jnp.where(lane == 1, odd, 0.0)).astype(bf)
    values[HEAD:] = jnp.ones((values.shape[0] - HEAD, n * rows), bf)

    @pl.when(outer)
    def _():
        landed(kv_in, n - 1, kv_r)

    landed(kv_out, n - 1, kv_s)
    for i in range(3):
        send_q(i)

    @pl.when(jnp.logical_not(outer))
    def _():
        landed(kv_in, n - 1, kv_r)

    for p in range(steps):
        both = jnp.concatenate([kv_in[2 * p, :HEAD], kv_in[2 * p + 1, :HEAD]], axis=0)
        keys[p * rows:(p + 1) * rows, :LANES] = both.T
        values[:HEAD, p * rows:(p + 1) * rows] = kv_in[2 * p, HEAD:]
        values[:HEAD, span + p * rows:span + (p + 1) * rows] = kv_in[2 * p + 1, HEAD:]

    chip = lax.div(me, 2)

    def chip_of(k):
        mask = jnp.where(k <= 1, 1 - k, jnp.where(k >= 5, k, jnp.where(k == 3, 4, lax.div(k, 2) + 1)))
        c0, c1, c2 = lax.rem(chip, 2), lax.rem(lax.div(chip, 2), 2), lax.div(chip, 4)
        k0, k1, k2 = lax.rem(mask, 2), lax.rem(lax.div(mask, 2), 2), lax.div(mask, 4)
        return 4 * flip(c2, k2) + 2 * flip(c1, k1) + flip(c0, k0)

    own_weight = jnp.where(cfg == 0, GUIDANCE, 1.0 - GUIDANCE)
    far_weight = 1.0 - own_weight

    def give(k):
        pair = chip_of(k)
        base = 2 * pair
        part = att_far.at[pl.ds(base, 2)]
        pltpu.make_async_copy(part, part, x_r.at[pair]).wait()
        for i in range(2):
            blend = own_weight * att_own[base + i].astype(f32) + far_weight * att_far[base + i].astype(f32)
            mixed[base + i] = blend.astype(bf)
            send(mixed, att_in, base + i, a_s, a_r.at[plane])

    row = lax.broadcasted_iota(jnp.int32, (LANES, 2 * rows), 0)
    first_row = jnp.where(row == 0, 1.0, 0.0).astype(bf)
    second_row = jnp.where(row == 1, 1.0, 0.0).astype(bf)
    blank = jnp.zeros((HEAD, 2 * rows), bf)

    def score(k, held):
        base = 2 * chip_of(jnp.minimum(k, steps - 1))
        for i in range(2):
            @pl.when(jnp.logical_and(base + i != me, k < steps))
            def _():
                pltpu.make_async_copy(q_in.at[base + i], q_in.at[base + i], q_r.at[base + i]).wait()
        query = jnp.concatenate([q_in[base], q_in[base + 1]], axis=1)
        upper = jnp.concatenate([query, blank, first_row], axis=0)
        lower = jnp.concatenate([blank, query, second_row], axis=0)
        even = jnp.dot(keys[...], upper, preferred_element_type=f32)
        odd = jnp.dot(keys[...], lower, preferred_element_type=f32)
        held[:span] = even
        held[span:] = odd
        return jnp.maximum(jnp.max(even, axis=0, keepdims=True), jnp.max(odd, axis=0, keepdims=True))

    def weigh(k, held, highest):
        pair = chip_of(k)
        base = 2 * pair
        numer = None
        for c in range(0, n * rows, 2 * rows):
            part = jnp.exp(held[c:c + 2 * rows] - highest).astype(bf)
            term = jnp.dot(values[:, c:c + 2 * rows], part, preferred_element_type=f32)
            numer = term if numer is None else numer + term
        result = (numer[:HEAD] / numer[HEAD:HEAD + 1]).astype(bf)
        att_own[base] = result[:, :rows]
        att_own[base + 1] = result[:, rows:]
        pltpu.make_async_remote_copy(
            src_ref=att_own.at[pl.ds(base, 2)], dst_ref=att_far.at[pl.ds(base, 2)],
            send_sem=x_s, recv_sem=x_r.at[pair],
            device_id={"cfg": 1 - cfg}, device_id_type=MESH).start()

    lag = 4

    def attend(i, highest):
        for part in range(2):
            k = 2 * i + part
            held, later = (held_a, held_b) if part == 0 else (held_b, held_a)
            following = score(k + 1, later)
            weigh(k, held, highest)
            highest = following

            @pl.when(k >= lag)
            def _():
                give(k - lag)

        return highest

    lax.fori_loop(0, steps // 2, attend, score(0, held_a))
    for k in range(steps - lag, steps):
        give(k)

    near = jnp.where(outer, 0, 2)
    order = (3, near, lax.rem(near + 1, 3), lax.rem(near + 2, 3))
    total = None
    for i in order:
        g = group(i)
        landed(att_in, heads_here - 1 if i is order[0] else heads_here, a_r.at[g])
        part = att_in[pl.ds(g * heads_here, heads_here)].reshape(cols, rows)
        term = jnp.dot(wo_turned[g], part, preferred_element_type=f32)
        total = term if total is None else total + term
    out_ref[...] = gate[...] * total

    landed(q_out, n - 1, q_s)
    landed(place_in, n - 1, p_s)
    landed(att_own, n, x_s)
    landed(mixed, n - 1, a_s)


def whole_kernel(hidden, modulation, w_qkv, q_gain, k_gain, w_out, text_count, block_order):
    n = lax.axis_size("seq")
    states = hidden[0]
    rows, width = states.shape
    features = w_out.shape[0]
    cols = features // GROUPS
    half = width // 2
    wide = -(-half // LANES) * LANES
    bf, f32 = jnp.bfloat16, jnp.float32
    hbm = pl.BlockSpec(memory_space=pltpu.HBM)
    dma = pltpu.SemaphoreType.DMA
    turned = pl.pallas_call(
        functools.partial(fused, n),
        out_shape=jax.ShapeDtypeStruct((half, rows), f32),
        in_specs=[pl.BlockSpec(memory_space=pltpu.SMEM)] + [hbm] * 6,
        out_specs=pl.BlockSpec(memory_space=pltpu.VMEM),
        scratch_shapes=[
            pltpu.VMEM((rows, width), bf),
            pltpu.VMEM(modulation.shape, f32),
            pltpu.VMEM((1, HEAD), f32),
            pltpu.VMEM((1, HEAD), f32),
            pltpu.VMEM((3, GROUPS, width, cols), bf),
            pltpu.VMEM((features, wide), bf),
            pltpu.VMEM((GROUPS, half, cols), bf),
            pltpu.VMEM((half, rows), f32),
            pltpu.VMEM((rows, width), bf),
            pltpu.VMEM((n, 2 * HEAD, rows), bf),
            pltpu.VMEM((n, 2 * HEAD, rows), bf),
            pltpu.VMEM((n, HEAD, rows), bf),
            pltpu.VMEM((n, HEAD, rows), bf),
            pltpu.VMEM((1, 1, LANES), jnp.int32),
            pltpu.VMEM((n, 1, LANES), jnp.int32),
            pltpu.VMEM((n * rows // 2, 2 * LANES), bf),
            pltpu.VMEM((HEAD + 16, n * rows), bf),
        ] + [pltpu.VMEM((n, HEAD, rows), bf)] * 4 + [pltpu.VMEM((n * rows, 2 * rows), f32)] * 2 + [
            dma((4,)), dma((3, GROUPS)), dma,
            dma, dma, dma, dma((n,)), dma, dma, dma, dma((n // 2,)), dma, dma((GROUPS,)),
        ],
        compiler_params=pltpu.CompilerParams(
            collective_id=0, has_side_effects=True, vmem_limit_bytes=40 * 1024 * 1024),
    )(block_order * SHIFT + text_count, *[pltpu.with_memory_space_constraint(x, pltpu.HBM) for x in (
        states, modulation, w_qkv, q_gain[None], k_gain[None], w_out)])
    return turned.T


def solution(mesh):
    in_specs = (P("cfg", "seq", None), P(), P(), P(), P(), P(), P("cfg"), P("seq"))
    out_specs = P("seq", "cfg")
    one_head_each = mesh.shape["seq"] == HEADS and mesh.shape["cfg"] == 2
    body = whole_kernel if one_head_each else shards
    return jax.shard_map(body, mesh=mesh, in_specs=in_specs, out_specs=out_specs, check_vma=False)
```

```python
import functools

import jax
import jax.numpy as jnp
from jax import lax
from jax.experimental import pallas as pl
from jax.experimental.pallas import tpu as pltpu
from jax.sharding import PartitionSpec as P

HEAD = 64
HEADS = 16
TXT = 226


GUIDANCE = 6.0
EPSILON = 1e-05
MASKED = -1000000000.0


def swapped(block, axis, apart):
    count = lax.axis_size(axis)
    route = []
    for low in range(count):
        high = low | 1 << apart
        if high != low and high < count:
            route += [(low, high), (high, low)]
    return lax.ppermute(block, axis, route)


def layer_normal(values_in):
    average = jnp.mean(values_in, axis=-1, keepdims=True)
    centred = values_in - average
    spread = jnp.mean(centred * centred, axis=-1, keepdims=True)
    return centred * lax.rsqrt(spread + EPSILON)


def modulated(states, is_text, modulation):
    normed = layer_normal(states.astype(jnp.float32))
    shift = jnp.where(is_text[:, None], modulation[3][None, :], modulation[0][None, :])
    scale = jnp.where(is_text[:, None], modulation[4][None, :], modulation[1][None, :])
    return (normed * (1.0 + scale) + shift).astype(jnp.bfloat16)


def head_normal(projected, gain):
    rows = projected.shape[0]
    heads_view = projected.reshape(rows, HEADS, HEAD)
    return (layer_normal(heads_view) * gain).reshape(rows, HEADS * HEAD).astype(jnp.bfloat16)


def projections(states, is_text, modulation, w_qkv, q_gain, k_gain):
    modded = modulated(states, is_text, modulation)
    query = head_normal(jnp.dot(modded, w_qkv[0], preferred_element_type=jnp.float32), q_gain)
    keys = head_normal(jnp.dot(modded, w_qkv[1], preferred_element_type=jnp.float32), k_gain)
    values = jnp.dot(modded, w_qkv[2], preferred_element_type=jnp.float32).astype(jnp.bfloat16)
    return (query, keys, values)


def fold_block(query_heads, carry, piece):
    highest, total, numer = carry
    keys_piece, values_piece, bias_piece = piece
    count = keys_piece.shape[0]
    key_heads = keys_piece.reshape(count, HEADS, HEAD)
    value_heads = values_piece.reshape(count, HEADS, HEAD)
    scores = jnp.einsum("qhd,khd->hqk", query_heads, key_heads, preferred_element_type=jnp.float32)
    scores = scores * HEAD ** (-0.5) + bias_piece.astype(jnp.float32)[None, None, :]
    new_high = jnp.maximum(highest, jnp.max(scores, axis=-1))
    expo = jnp.exp(scores - new_high[:, :, None])
    rescale = jnp.exp(highest - new_high)
    total = jnp.sum(expo, axis=-1)
    numer = numer * rescale.T[:, :, None] + jnp.einsum(
        "hqk,khd->qhd", expo.astype(jnp.bfloat16), value_heads, preferred_element_type=jnp.float32
    )
    return (new_high, total, numer)


def shards(hidden, modulation, w_qkv, q_gain, k_gain, w_out, text_count, block_order):
    states = hidden[0]
    tok_rows = states.shape[0]
    within = jnp.arange(tok_rows, dtype=jnp.int32)
    position = block_order[0] * tok_rows + within
    is_text = position < TXT
    keep = jnp.logical_or(position >= TXT, position < text_count[0])
    key_bias = jnp.where(keep, 0.0, MASKED).astype(jnp.bfloat16)
    query, keys, values = projections(states, is_text, modulation, w_qkv, q_gain, k_gain)
    query_heads = query.reshape(tok_rows, HEADS, HEAD)
    start_state = (
        jnp.full((HEADS, tok_rows), -1e30, jnp.float32),
        jnp.zeros((HEADS, tok_rows), jnp.float32),
        jnp.zeros((tok_rows, HEADS, HEAD), jnp.float32),
    )
    carry = fold_block(
        query_heads,
        start_state,
        (
            lax.all_gather(keys, "seq", axis=0, tiled=True),
            lax.all_gather(values, "seq", axis=0, tiled=True),
            lax.all_gather(key_bias, "seq", axis=0, tiled=True),
        ),
    )
    highest, total, numer = carry
    attended = (numer / total.T[:, :, None]).reshape(tok_rows, HEADS * HEAD).astype(jnp.bfloat16)
    gate = jnp.where(is_text[:, None], modulation[5][None, :], modulation[2][None, :])
    cfg_index = lax.axis_index("cfg")
    half_width = w_out.shape[1] // 2
    w_half = lax.dynamic_slice_in_dim(w_out, cfg_index * half_width, half_width, 1)
    gate_half = lax.dynamic_slice_in_dim(gate, cfg_index * half_width, half_width, 1)
    partner = swapped(attended, "cfg", 0)
    own_update = gate_half * jnp.dot(attended, w_half, preferred_element_type=jnp.float32)
    other_update = gate_half * jnp.dot(partner, w_half, preferred_element_type=jnp.float32)
    is_first = cfg_index == 0
    cond = jnp.where(is_first, own_update, other_update)
    uncond = jnp.where(is_first, other_update, own_update)
    return uncond + GUIDANCE * (cond - uncond)


LANES = 128
GROUPS = 4
SHIFT = 256
ORDER = (1, 0, 2, 4, 3, 5, 6, 7)
MESH = pl.DeviceIdType.MESH


def flip(bit, other):
    return lax.rem(bit + other, 2)


def column_normal(x):
    centred = x - jnp.mean(x, axis=0, keepdims=True)
    spread = jnp.mean(centred * centred, axis=0, keepdims=True)
    return centred * lax.rsqrt(spread + EPSILON)


def fused(n, info_ref, hidden_ref, mod_ref, w_ref, qg_ref, kg_ref, wo_ref, out_ref,
          hidden_v, mod_v, qg_v, kg_v, w_buf, wo_buf, wo_turned, gate, modded,
          kv_out, kv_in, q_out, q_in, place_out, place_in, keys, values,
          att_own, att_far, mixed, att_in, held_a, held_b,
          in_sem, w_sem, wo_sem, kv_s, kv_r, q_s, q_r, p_s, p_r, x_s, x_r, a_s, a_r):
    me = lax.axis_index("seq")
    cfg = lax.axis_index("cfg")
    rows, width = hidden_ref.shape
    half = width // 2
    wide = wo_buf.shape[1]
    excess = wide - half
    cols = w_buf.shape[3]
    heads_here = cols // HEAD
    steps = n // 2
    span = n * rows // 2
    bf, f32 = jnp.bfloat16, jnp.float32
    plane = lax.div(me, GROUPS)
    plane_high, plane_low = lax.div(plane, 2), lax.rem(plane, 2)
    side, core = lax.rem(lax.div(me, 2), 2), lax.rem(me, 2)

    barrier = pltpu.get_barrier_semaphore()
    for j in range(1, n):
        pl.semaphore_signal(barrier, inc=1, device_id={"seq": lax.rem(me + j, n)}, device_id_type=MESH)
    pl.semaphore_signal(barrier, inc=1, device_id={"cfg": 1 - cfg}, device_id_type=MESH)

    outer = plane_high == plane_low

    def plane_at(mask):
        return 2 * flip(plane_high, mask // 2) + flip(plane_low, mask % 2)

    def group(i):
        mask = jnp.where(outer, lax.rem(i + 1, GROUPS), jnp.where(i == 3, 0, lax.rem(i + 1, 3) + 1))
        return plane_at(mask)

    def member(first, h):
        return first + 2 * flip(side, h // 2) + flip(core, h % 2)

    def weight(kind, i):
        start = pl.multiple_of(group(i) * cols, cols)
        return pltpu.make_async_copy(
            w_ref.at[kind, :, pl.ds(start, cols)], w_buf.at[kind, i], w_sem.at[kind, i])

    column = pl.multiple_of(cfg * (width - wide), LANES)
    out_weight = pltpu.make_async_copy(wo_ref.at[:, pl.ds(column, wide)], wo_buf, wo_sem)
    inputs = [pltpu.make_async_copy(a, b, in_sem.at[i]) for i, (a, b) in enumerate([
        (hidden_ref, hidden_v), (mod_ref, mod_v),
        (kg_ref, kg_v), (qg_ref, qg_v)])]
    for copy in inputs:
        copy.start()
    weight(1, 0).start()
    weight(2, 0).start()

    def send(src, dst, to, s_sem, r_sem):
        @pl.when(to != me)
        def _():
            pltpu.make_async_remote_copy(
                src_ref=src.at[to], dst_ref=dst.at[me], send_sem=s_sem, recv_sem=r_sem,
                device_id={"seq": to}, device_id_type=MESH).start()

        @pl.when(to == me)
        def _():
            dst[me] = src[to]

    def landed(ref, count, sem):
        part = ref.at[pl.ds(0, count)]
        pltpu.make_async_copy(part, part, sem).wait()

    for copy in inputs:
        copy.wait()
    block = lax.div(info_ref[0], SHIFT)
    count = lax.rem(info_ref[0], SHIFT)
    mod = mod_v[...]
    down = block * rows + lax.broadcasted_iota(jnp.int32, (rows, 1), 0)
    is_text = down < TXT
    normed = layer_normal(hidden_v[...].astype(f32))
    shift = jnp.where(is_text, mod[3:4, :], mod[0:1, :])
    scale = jnp.where(is_text, mod[4:5, :], mod[1:2, :])
    modded[...] = (normed * (1.0 + scale) + shift).astype(bf)

    for i in range(1, GROUPS):
        weight(1, i).start()
        weight(2, i).start()
    for i in range(GROUPS):
        weight(0, i).start()
    out_weight.start()

    def down_lanes(gain_row):
        both = jnp.concatenate([gain_row, gain_row], axis=1)
        return jnp.broadcast_to(both, (LANES, LANES)).T[:HEAD]

    k_gain = down_lanes(kg_v[...])
    q_gain = down_lanes(qg_v[...]) * HEAD ** (-0.5)
    place_out[0] = jnp.full((1, LANES), block, jnp.int32)
    place_in[me] = jnp.full((1, LANES), block, jnp.int32)

    def project_kv(i):
        weight(1, i).wait()
        weight(2, i).wait()
        first = group(i) * heads_here
        x = modded[...]
        k_all = jnp.dot(x, w_buf[1, i], preferred_element_type=f32).T
        v_all = jnp.dot(x, w_buf[2, i], preferred_element_type=f32).T
        for h in range(heads_here):
            part = slice(h * HEAD, (h + 1) * HEAD)
            kv_out[first + h, :HEAD] = (column_normal(k_all[part]) * k_gain).astype(bf)
            kv_out[first + h, HEAD:] = v_all[part].astype(bf)

    def send_kv(i):
        if isinstance(i, int):
            pl.semaphore_wait(barrier, n)
            for j in range(1, n):
                pltpu.make_async_remote_copy(
                    src_ref=place_out.at[0], dst_ref=place_in.at[me], send_sem=p_s, recv_sem=p_r,
                    device_id={"seq": lax.rem(me + j, n)}, device_id_type=MESH).start()
        for h in range(heads_here):
            send(kv_out, kv_in, member(group(i) * heads_here, h), kv_s, kv_r)

    def rest_kv(i, carry):
        project_kv(i)
        send_kv(i)
        return carry

    project_kv(0)
    send_kv(0)
    lax.fori_loop(1, GROUPS, rest_kv, 0)

    def project_q(i):
        weight(0, i).wait()
        first = group(i) * heads_here
        q_all = jnp.dot(modded[...], w_buf[0, i], preferred_element_type=f32).T
        for h in range(heads_here):
            part = slice(h * HEAD, (h + 1) * HEAD)
            q_out[first + h] = (column_normal(q_all[part]) * q_gain).astype(bf)

    def send_q(mask):
        for h in range(heads_here):
            send(q_out, q_in, member(plane_at(mask) * heads_here, h), q_s.at[mask], q_r.at[me])

    lax.fori_loop(0, GROUPS, lambda i, carry: (project_q(i), carry)[1], 0)
    send_q(0)

    out_weight.wait()

    def put(target, turned, c):
        @pl.when(cfg == 0)
        def _():
            low, high = c * LANES, min((c + 1) * LANES, half)
            target[low:high] = turned[:high - low]

        @pl.when(cfg != 0)
        def _():
            low, high = max(c * LANES - excess, 0), (c + 1) * LANES - excess
            target[low:high] = turned[LANES - (high - low):]

    gate_text = jnp.where(cfg == 0, mod_v[5:6, :wide], mod_v[5:6, width - wide:])
    gate_video = jnp.where(cfg == 0, mod_v[2:3, :wide], mod_v[2:3, width - wide:])
    for c in range(wide // LANES):
        part = slice(c * LANES, (c + 1) * LANES)
        put(gate, jnp.where(is_text, gate_text[:, part], gate_video[:, part]).T, c)
        for g in range(GROUPS):
            put(wo_turned.at[g], wo_buf[g * cols:(g + 1) * cols, part].T, c)

    landed(place_in, n - 1, p_r)
    lane = lax.broadcasted_iota(jnp.int32, (rows, LANES), 1)
    sub = lax.broadcasted_iota(jnp.int32, (rows, LANES), 0)

    def masked(j):
        at = place_in[j] * rows + sub
        return jnp.where(jnp.logical_or(at >= TXT, at < count), 0.0, MASKED)

    for p in range(steps):
        even, odd = masked(2 * p), masked(2 * p + 1)
        keys[p * rows:(p + 1) * rows, LANES:] = jnp.where(
            lane == 0, even, jnp.where(lane == 1, odd, 0.0)).astype(bf)
    values[HEAD:] = jnp.ones((values.shape[0] - HEAD, n * rows), bf)

    @pl.when(outer)
    def _():
        landed(kv_in, n - 1, kv_r)

    landed(kv_out, n - 1, kv_s)
    send_q(1)
    send_q(2)
    send_q(3)

    @pl.when(jnp.logical_not(outer))
    def _():
        landed(kv_in, n - 1, kv_r)

    for p in range(steps):
        both = jnp.concatenate([kv_in[2 * p, :HEAD], kv_in[2 * p + 1, :HEAD]], axis=0)
        keys[p * rows:(p + 1) * rows, :LANES] = both.T
        values[:HEAD, p * rows:(p + 1) * rows] = kv_in[2 * p, HEAD:]
        values[:HEAD, span + p * rows:span + (p + 1) * rows] = kv_in[2 * p + 1, HEAD:]

    chip = lax.div(me, 2)

    def chip_of(k):
        mask = sum(jnp.where(k == i, at, 0) for i, at in enumerate(ORDER))
        c0, c1, c2 = lax.rem(chip, 2), lax.rem(lax.div(chip, 2), 2), lax.div(chip, 4)
        k0, k1, k2 = lax.rem(mask, 2), lax.rem(lax.div(mask, 2), 2), lax.div(mask, 4)
        return 4 * flip(c2, k2) + 2 * flip(c1, k1) + flip(c0, k0)

    own_weight = jnp.where(cfg == 0, GUIDANCE, 1.0 - GUIDANCE)
    far_weight = 1.0 - own_weight

    def give(k):
        pair = chip_of(k)
        base = 2 * pair
        part = att_far.at[pl.ds(base, 2)]
        pltpu.make_async_copy(part, part, x_r.at[pair]).wait()
        for i in range(2):
            blend = own_weight * att_own[base + i].astype(f32) + far_weight * att_far[base + i].astype(f32)
            mixed[base + i] = blend.astype(bf)
            send(mixed, att_in, base + i, a_s, a_r.at[plane])

    row = lax.broadcasted_iota(jnp.int32, (LANES, 2 * rows), 0)
    first_row = jnp.where(row == 0, 1.0, 0.0).astype(bf)
    second_row = jnp.where(row == 1, 1.0, 0.0).astype(bf)
    blank = jnp.zeros((HEAD, 2 * rows), bf)

    def score(k, held):
        base = 2 * chip_of(k)
        for i in range(2):
            @pl.when(base + i != me)
            def _():
                pltpu.make_async_copy(q_in.at[base + i], q_in.at[base + i], q_r.at[base + i]).wait()
        query = jnp.concatenate([q_in[base], q_in[base + 1]], axis=1)
        upper = jnp.concatenate([query, blank, first_row], axis=0)
        lower = jnp.concatenate([blank, query, second_row], axis=0)
        even = jnp.dot(keys[...], upper, preferred_element_type=f32)
        odd = jnp.dot(keys[...], lower, preferred_element_type=f32)
        held[:span] = even
        held[span:] = odd
        return jnp.maximum(jnp.max(even, axis=0, keepdims=True), jnp.max(odd, axis=0, keepdims=True))

    def weigh(k, held, highest):
        pair = chip_of(k)
        base = 2 * pair
        numer = None
        for c in range(0, n * rows, 2 * rows):
            part = jnp.exp(held[c:c + 2 * rows] - highest).astype(bf)
            term = jnp.dot(values[:, c:c + 2 * rows], part, preferred_element_type=f32)
            numer = term if numer is None else numer + term
        result = (numer[:HEAD] / numer[HEAD:HEAD + 1]).astype(bf)
        att_own[base] = result[:, :rows]
        att_own[base + 1] = result[:, rows:]
        pltpu.make_async_remote_copy(
            src_ref=att_own.at[pl.ds(base, 2)], dst_ref=att_far.at[pl.ds(base, 2)],
            send_sem=x_s, recv_sem=x_r.at[pair],
            device_id={"cfg": 1 - cfg}, device_id_type=MESH).start()

    lag = 3

    def late_gift(k):
        @pl.when(k >= lag)
        def _():
            give(k - lag)

    def attend(i, highest):
        for part in range(2):
            k = 2 * i + part
            held, later = (held_a, held_b) if part == 0 else (held_b, held_a)
            following = score(k + 1, later)
            weigh(k, held, highest)
            highest = following
            late_gift(k)
        return highest

    highest = lax.fori_loop(0, steps // 2 - 1, attend, score(0, held_a))
    following = score(steps - 1, held_b)
    weigh(steps - 2, held_a, highest)
    give(steps - 2 - lag)
    weigh(steps - 1, held_b, following)
    give(steps - 1 - lag)
    for k in range(steps - lag, steps):
        give(k)

    for mask in range(GROUPS):
        landed(q_out, heads_here if mask else heads_here - 1, q_s.at[mask])
    landed(place_in, n - 1, p_s)
    landed(att_own, n, x_s)
    landed(mixed, n - 1, a_s)

    total = None
    for mask in (0, 1, 2, 3):
        g = plane_at(mask)
        landed(att_in, heads_here if mask else heads_here - 1, a_r.at[g])
        part = att_in[pl.ds(g * heads_here, heads_here)].reshape(cols, rows)
        term = jnp.dot(wo_turned[g], part, preferred_element_type=f32)
        total = term if total is None else total + term
    out_ref[...] = gate[...] * total


def whole_kernel(hidden, modulation, w_qkv, q_gain, k_gain, w_out, text_count, block_order):
    n = lax.axis_size("seq")
    states = hidden[0]
    rows, width = states.shape
    features = w_out.shape[0]
    cols = features // GROUPS
    half = width // 2
    wide = -(-half // LANES) * LANES
    bf, f32 = jnp.bfloat16, jnp.float32
    hbm = pl.BlockSpec(memory_space=pltpu.HBM)
    dma = pltpu.SemaphoreType.DMA
    turned = pl.pallas_call(
        functools.partial(fused, n),
        out_shape=jax.ShapeDtypeStruct((half, rows), f32),
        in_specs=[pl.BlockSpec(memory_space=pltpu.SMEM)] + [hbm] * 6,
        out_specs=pl.BlockSpec(memory_space=pltpu.VMEM),
        scratch_shapes=[
            pltpu.VMEM((rows, width), bf),
            pltpu.VMEM(modulation.shape, f32),
            pltpu.VMEM((1, HEAD), f32),
            pltpu.VMEM((1, HEAD), f32),
            pltpu.VMEM((3, GROUPS, width, cols), bf),
            pltpu.VMEM((features, wide), bf),
            pltpu.VMEM((GROUPS, half, cols), bf),
            pltpu.VMEM((half, rows), f32),
            pltpu.VMEM((rows, width), bf),
            pltpu.VMEM((n, 2 * HEAD, rows), bf),
            pltpu.VMEM((n, 2 * HEAD, rows), bf),
            pltpu.VMEM((n, HEAD, rows), bf),
            pltpu.VMEM((n, HEAD, rows), bf),
            pltpu.VMEM((1, 1, LANES), jnp.int32),
            pltpu.VMEM((n, 1, LANES), jnp.int32),
            pltpu.VMEM((n * rows // 2, 2 * LANES), bf),
            pltpu.VMEM((HEAD + 16, n * rows), bf),
        ] + [pltpu.VMEM((n, HEAD, rows), bf)] * 4 + [pltpu.VMEM((n * rows, 2 * rows), f32)] * 2 + [
            dma((4,)), dma((3, GROUPS)), dma,
            dma, dma, dma((GROUPS,)), dma((n,)), dma, dma, dma, dma((n // 2,)), dma, dma((GROUPS,)),
        ],
        compiler_params=pltpu.CompilerParams(
            collective_id=0, has_side_effects=True, vmem_limit_bytes=40 * 1024 * 1024),
    )(block_order * SHIFT + text_count, *[pltpu.with_memory_space_constraint(x, pltpu.HBM) for x in (
        states, modulation, w_qkv, q_gain[None], k_gain[None], w_out)])
    return turned.T


def solution(mesh):
    in_specs = (P("cfg", "seq", None), P(), P(), P(), P(), P(), P("cfg"), P("seq"))
    out_specs = P("seq", "cfg")
    one_head_each = mesh.shape["seq"] == HEADS and mesh.shape["cfg"] == 2
    body = whole_kernel if one_head_each else shards
    return jax.shard_map(body, mesh=mesh, in_specs=in_specs, out_specs=out_specs, check_vma=False)
```

```python
import functools

import jax
import jax.numpy as jnp
from jax import lax
from jax.experimental import pallas as pl
from jax.experimental.pallas import tpu as pltpu
from jax.sharding import PartitionSpec as P

HEAD = 64
HEADS = 16
TXT = 226


GUIDANCE = 6.0
EPSILON = 1e-05
MASKED = -1000000000.0


def swapped(block, axis, apart):
    count = lax.axis_size(axis)
    route = []
    for low in range(count):
        high = low | 1 << apart
        if high != low and high < count:
            route += [(low, high), (high, low)]
    return lax.ppermute(block, axis, route)


def layer_normal(values_in):
    average = jnp.mean(values_in, axis=-1, keepdims=True)
    centred = values_in - average
    spread = jnp.mean(centred * centred, axis=-1, keepdims=True)
    return centred * lax.rsqrt(spread + EPSILON)


def modulated(states, is_text, modulation):
    normed = layer_normal(states.astype(jnp.float32))
    shift = jnp.where(is_text[:, None], modulation[3][None, :], modulation[0][None, :])
    scale = jnp.where(is_text[:, None], modulation[4][None, :], modulation[1][None, :])
    return (normed * (1.0 + scale) + shift).astype(jnp.bfloat16)


def head_normal(projected, gain):
    rows = projected.shape[0]
    heads_view = projected.reshape(rows, HEADS, HEAD)
    return (layer_normal(heads_view) * gain).reshape(rows, HEADS * HEAD).astype(jnp.bfloat16)


def projections(states, is_text, modulation, w_qkv, q_gain, k_gain):
    modded = modulated(states, is_text, modulation)
    query = head_normal(jnp.dot(modded, w_qkv[0], preferred_element_type=jnp.float32), q_gain)
    keys = head_normal(jnp.dot(modded, w_qkv[1], preferred_element_type=jnp.float32), k_gain)
    values = jnp.dot(modded, w_qkv[2], preferred_element_type=jnp.float32).astype(jnp.bfloat16)
    return (query, keys, values)


def fold_block(query_heads, carry, piece):
    highest, total, numer = carry
    keys_piece, values_piece, bias_piece = piece
    count = keys_piece.shape[0]
    key_heads = keys_piece.reshape(count, HEADS, HEAD)
    value_heads = values_piece.reshape(count, HEADS, HEAD)
    scores = jnp.einsum("qhd,khd->hqk", query_heads, key_heads, preferred_element_type=jnp.float32)
    scores = scores * HEAD ** (-0.5) + bias_piece.astype(jnp.float32)[None, None, :]
    new_high = jnp.maximum(highest, jnp.max(scores, axis=-1))
    expo = jnp.exp(scores - new_high[:, :, None])
    rescale = jnp.exp(highest - new_high)
    total = jnp.sum(expo, axis=-1)
    numer = numer * rescale.T[:, :, None] + jnp.einsum(
        "hqk,khd->qhd", expo.astype(jnp.bfloat16), value_heads, preferred_element_type=jnp.float32
    )
    return (new_high, total, numer)


def shards(hidden, modulation, w_qkv, q_gain, k_gain, w_out, text_count, block_order):
    states = hidden[0]
    tok_rows = states.shape[0]
    within = jnp.arange(tok_rows, dtype=jnp.int32)
    position = block_order[0] * tok_rows + within
    is_text = position < TXT
    keep = jnp.logical_or(position >= TXT, position < text_count[0])
    key_bias = jnp.where(keep, 0.0, MASKED).astype(jnp.bfloat16)
    query, keys, values = projections(states, is_text, modulation, w_qkv, q_gain, k_gain)
    query_heads = query.reshape(tok_rows, HEADS, HEAD)
    start_state = (
        jnp.full((HEADS, tok_rows), -1e30, jnp.float32),
        jnp.zeros((HEADS, tok_rows), jnp.float32),
        jnp.zeros((tok_rows, HEADS, HEAD), jnp.float32),
    )
    carry = fold_block(
        query_heads,
        start_state,
        (
            lax.all_gather(keys, "seq", axis=0, tiled=True),
            lax.all_gather(values, "seq", axis=0, tiled=True),
            lax.all_gather(key_bias, "seq", axis=0, tiled=True),
        ),
    )
    highest, total, numer = carry
    attended = (numer / total.T[:, :, None]).reshape(tok_rows, HEADS * HEAD).astype(jnp.bfloat16)
    gate = jnp.where(is_text[:, None], modulation[5][None, :], modulation[2][None, :])
    cfg_index = lax.axis_index("cfg")
    half_width = w_out.shape[1] // 2
    w_half = lax.dynamic_slice_in_dim(w_out, cfg_index * half_width, half_width, 1)
    gate_half = lax.dynamic_slice_in_dim(gate, cfg_index * half_width, half_width, 1)
    partner = swapped(attended, "cfg", 0)
    own_update = gate_half * jnp.dot(attended, w_half, preferred_element_type=jnp.float32)
    other_update = gate_half * jnp.dot(partner, w_half, preferred_element_type=jnp.float32)
    is_first = cfg_index == 0
    cond = jnp.where(is_first, own_update, other_update)
    uncond = jnp.where(is_first, other_update, own_update)
    return uncond + GUIDANCE * (cond - uncond)


LANES = 128
GROUPS = 4
SHIFT = 256
ORDER = (1, 0, 2, 4, 3, 5, 6, 7)
MESH = pl.DeviceIdType.MESH


def flip(bit, other):
    return lax.rem(bit + other, 2)


def column_normal(x):
    centred = x - jnp.mean(x, axis=0, keepdims=True)
    spread = jnp.mean(centred * centred, axis=0, keepdims=True)
    return centred * lax.rsqrt(spread + EPSILON)


def fused(n, info_ref, hidden_ref, mod_ref, w_ref, qg_ref, kg_ref, wo_ref, out_ref,
          hidden_v, mod_v, qg_v, kg_v, w_buf, wo_buf, wo_turned, gate, modded,
          kv_out, kv_in, q_out, q_in, place_out, place_in, keys, values,
          att_own, att_far, mixed, att_in, held_a, held_b,
          in_sem, w_sem, wo_sem, kv_s, kv_r, q_s, q_r, p_s, p_r, x_s, x_r, a_s, a_r):
    me = lax.axis_index("seq")
    cfg = lax.axis_index("cfg")
    rows, width = hidden_ref.shape
    half = width // 2
    wide = wo_buf.shape[1]
    excess = wide - half
    cols = w_buf.shape[3]
    heads_here = cols // HEAD
    steps = n // 2
    span = n * rows // 2
    bf, f32 = jnp.bfloat16, jnp.float32
    plane = lax.div(me, GROUPS)
    plane_high, plane_low = lax.div(plane, 2), lax.rem(plane, 2)
    side, core = lax.rem(lax.div(me, 2), 2), lax.rem(me, 2)

    barrier = pltpu.get_barrier_semaphore()
    for j in range(1, n):
        pl.semaphore_signal(barrier, inc=1, device_id={"seq": lax.rem(me + j, n)}, device_id_type=MESH)
    pl.semaphore_signal(barrier, inc=1, device_id={"cfg": 1 - cfg}, device_id_type=MESH)

    outer = plane_high == plane_low

    def plane_at(mask):
        return 2 * flip(plane_high, mask // 2) + flip(plane_low, mask % 2)

    def group(i):
        mask = jnp.where(i == 3, 0, lax.rem(i + 1, 3) + 1)
        return plane_at(mask)

    def member(first, h):
        return first + 2 * flip(side, h // 2) + flip(core, h % 2)

    def weight(kind, i):
        start = pl.multiple_of(group(i) * cols, cols)
        return pltpu.make_async_copy(
            w_ref.at[kind, :, pl.ds(start, cols)], w_buf.at[kind, i], w_sem.at[kind, i])

    column = pl.multiple_of(cfg * (width - wide), LANES)
    out_weight = pltpu.make_async_copy(wo_ref.at[:, pl.ds(column, wide)], wo_buf, wo_sem)
    inputs = [pltpu.make_async_copy(a, b, in_sem.at[i]) for i, (a, b) in enumerate([
        (hidden_ref, hidden_v), (mod_ref, mod_v),
        (kg_ref, kg_v), (qg_ref, qg_v)])]
    for copy in inputs:
        copy.start()
    weight(1, 0).start()
    weight(2, 0).start()

    def send(src, dst, to, s_sem, r_sem):
        @pl.when(to != me)
        def _():
            pltpu.make_async_remote_copy(
                src_ref=src.at[to], dst_ref=dst.at[me], send_sem=s_sem, recv_sem=r_sem,
                device_id={"seq": to}, device_id_type=MESH).start()

        @pl.when(to == me)
        def _():
            dst[me] = src[to]

    def landed(ref, count, sem):
        part = ref.at[pl.ds(0, count)]
        pltpu.make_async_copy(part, part, sem).wait()

    for copy in inputs:
        copy.wait()
    block = lax.div(info_ref[0], SHIFT)
    count = lax.rem(info_ref[0], SHIFT)
    mod = mod_v[...]
    down = block * rows + lax.broadcasted_iota(jnp.int32, (rows, 1), 0)
    is_text = down < TXT
    normed = layer_normal(hidden_v[...].astype(f32))
    shift = jnp.where(is_text, mod[3:4, :], mod[0:1, :])
    scale = jnp.where(is_text, mod[4:5, :], mod[1:2, :])
    modded[...] = (normed * (1.0 + scale) + shift).astype(bf)

    for i in range(1, GROUPS):
        weight(1, i).start()
        weight(2, i).start()
    for i in range(GROUPS):
        weight(0, i).start()
    out_weight.start()

    def down_lanes(gain_row):
        both = jnp.concatenate([gain_row, gain_row], axis=1)
        return jnp.broadcast_to(both, (LANES, LANES)).T[:HEAD]

    k_gain = down_lanes(kg_v[...])
    q_gain = down_lanes(qg_v[...]) * HEAD ** (-0.5)
    place_out[0] = jnp.full((1, LANES), block, jnp.int32)
    place_in[me] = jnp.full((1, LANES), block, jnp.int32)

    def project_kv(i):
        weight(1, i).wait()
        weight(2, i).wait()
        first = group(i) * heads_here
        x = modded[...]
        k_all = jnp.dot(x, w_buf[1, i], preferred_element_type=f32).T
        v_all = jnp.dot(x, w_buf[2, i], preferred_element_type=f32).T
        for h in range(heads_here):
            part = slice(h * HEAD, (h + 1) * HEAD)
            kv_out[first + h, :HEAD] = (column_normal(k_all[part]) * k_gain).astype(bf)
            kv_out[first + h, HEAD:] = v_all[part].astype(bf)

    def send_kv(i):
        if isinstance(i, int):
            pl.semaphore_wait(barrier, n)
            for j in range(1, n):
                pltpu.make_async_remote_copy(
                    src_ref=place_out.at[0], dst_ref=place_in.at[me], send_sem=p_s, recv_sem=p_r,
                    device_id={"seq": lax.rem(me + j, n)}, device_id_type=MESH).start()
        for h in range(heads_here):
            send(kv_out, kv_in, member(group(i) * heads_here, h), kv_s, kv_r)

    def rest_kv(i, carry):
        project_kv(i)
        send_kv(i)
        return carry

    project_kv(0)
    send_kv(0)
    lax.fori_loop(1, GROUPS, rest_kv, 0)

    def project_q(i):
        weight(0, i).wait()
        first = group(i) * heads_here
        q_all = jnp.dot(modded[...], w_buf[0, i], preferred_element_type=f32).T
        for h in range(heads_here):
            part = slice(h * HEAD, (h + 1) * HEAD)
            q_out[first + h] = (column_normal(q_all[part]) * q_gain).astype(bf)

    def send_q(mask):
        for h in range(heads_here):
            send(q_out, q_in, member(plane_at(mask) * heads_here, h), q_s.at[mask], q_r.at[me])

    lax.fori_loop(0, GROUPS, lambda i, carry: (project_q(i), carry)[1], 0)
    send_q(0)

    out_weight.wait()

    def put(target, turned, c):
        @pl.when(cfg == 0)
        def _():
            low, high = c * LANES, min((c + 1) * LANES, half)
            target[low:high] = turned[:high - low]

        @pl.when(cfg != 0)
        def _():
            low, high = max(c * LANES - excess, 0), (c + 1) * LANES - excess
            target[low:high] = turned[LANES - (high - low):]

    gate_text = jnp.where(cfg == 0, mod_v[5:6, :wide], mod_v[5:6, width - wide:])
    gate_video = jnp.where(cfg == 0, mod_v[2:3, :wide], mod_v[2:3, width - wide:])
    for c in range(wide // LANES):
        part = slice(c * LANES, (c + 1) * LANES)
        put(gate, jnp.where(is_text, gate_text[:, part], gate_video[:, part]).T, c)
        for g in range(GROUPS):
            put(wo_turned.at[g], wo_buf[g * cols:(g + 1) * cols, part].T, c)

    landed(place_in, n - 1, p_r)
    lane = lax.broadcasted_iota(jnp.int32, (rows, LANES), 1)
    sub = lax.broadcasted_iota(jnp.int32, (rows, LANES), 0)

    def masked(j):
        at = place_in[j] * rows + sub
        return jnp.where(jnp.logical_or(at >= TXT, at < count), 0.0, MASKED)

    for p in range(steps):
        even, odd = masked(2 * p), masked(2 * p + 1)
        keys[p * rows:(p + 1) * rows, LANES:] = jnp.where(
            lane == 0, even, jnp.where(lane == 1, odd, 0.0)).astype(bf)
    values[HEAD:] = jnp.ones((values.shape[0] - HEAD, n * rows), bf)

    @pl.when(outer)
    def _():
        landed(kv_in, n - 1, kv_r)

    landed(kv_out, n - 1, kv_s)
    send_q(1)
    send_q(2)
    send_q(3)

    @pl.when(jnp.logical_not(outer))
    def _():
        landed(kv_in, n - 1, kv_r)

    for p in range(steps):
        both = jnp.concatenate([kv_in[2 * p, :HEAD], kv_in[2 * p + 1, :HEAD]], axis=0)
        keys[p * rows:(p + 1) * rows, :LANES] = both.T
        values[:HEAD, p * rows:(p + 1) * rows] = kv_in[2 * p, HEAD:]
        values[:HEAD, span + p * rows:span + (p + 1) * rows] = kv_in[2 * p + 1, HEAD:]

    chip = lax.div(me, 2)

    def chip_of(k):
        mask = sum(jnp.where(k == i, at, 0) for i, at in enumerate(ORDER))
        c0, c1, c2 = lax.rem(chip, 2), lax.rem(lax.div(chip, 2), 2), lax.div(chip, 4)
        k0, k1, k2 = lax.rem(mask, 2), lax.rem(lax.div(mask, 2), 2), lax.div(mask, 4)
        return 4 * flip(c2, k2) + 2 * flip(c1, k1) + flip(c0, k0)

    own_weight = jnp.where(cfg == 0, GUIDANCE, 1.0 - GUIDANCE)
    far_weight = 1.0 - own_weight

    def give(k):
        pair = chip_of(k)
        base = 2 * pair
        part = att_far.at[pl.ds(base, 2)]
        pltpu.make_async_copy(part, part, x_r.at[pair]).wait()
        for i in range(2):
            blend = own_weight * att_own[base + i].astype(f32) + far_weight * att_far[base + i].astype(f32)
            mixed[base + i] = blend.astype(bf)
            send(mixed, att_in, base + i, a_s, a_r.at[plane])

    row = lax.broadcasted_iota(jnp.int32, (LANES, 2 * rows), 0)
    first_row = jnp.where(row == 0, 1.0, 0.0).astype(bf)
    second_row = jnp.where(row == 1, 1.0, 0.0).astype(bf)
    blank = jnp.zeros((HEAD, 2 * rows), bf)

    def score(k, held):
        base = 2 * chip_of(k)
        for i in range(2):
            @pl.when(base + i != me)
            def _():
                pltpu.make_async_copy(q_in.at[base + i], q_in.at[base + i], q_r.at[base + i]).wait()
        query = jnp.concatenate([q_in[base], q_in[base + 1]], axis=1)
        upper = jnp.concatenate([query, blank, first_row], axis=0)
        lower = jnp.concatenate([blank, query, second_row], axis=0)
        even = jnp.dot(keys[...], upper, preferred_element_type=f32)
        odd = jnp.dot(keys[...], lower, preferred_element_type=f32)
        held[:span] = even
        held[span:] = odd
        return jnp.maximum(jnp.max(even, axis=0, keepdims=True), jnp.max(odd, axis=0, keepdims=True))

    def weigh(k, held, highest):
        pair = chip_of(k)
        base = 2 * pair
        numer = None
        for c in range(0, n * rows, 2 * rows):
            part = jnp.exp(held[c:c + 2 * rows] - highest).astype(bf)
            term = jnp.dot(values[:, c:c + 2 * rows], part, preferred_element_type=f32)
            numer = term if numer is None else numer + term
        result = (numer[:HEAD] / numer[HEAD:HEAD + 1]).astype(bf)
        att_own[base] = result[:, :rows]
        att_own[base + 1] = result[:, rows:]
        pltpu.make_async_remote_copy(
            src_ref=att_own.at[pl.ds(base, 2)], dst_ref=att_far.at[pl.ds(base, 2)],
            send_sem=x_s, recv_sem=x_r.at[pair],
            device_id={"cfg": 1 - cfg}, device_id_type=MESH).start()

    lag = 3

    def late_gift(k):
        @pl.when(k >= lag)
        def _():
            give(k - lag)

    def attend(i, highest):
        for part in range(2):
            k = 2 * i + part
            held, later = (held_a, held_b) if part == 0 else (held_b, held_a)
            following = score(k + 1, later)
            weigh(k, held, highest)
            highest = following
            late_gift(k)
        return highest

    highest = lax.fori_loop(0, steps // 2 - 1, attend, score(0, held_a))
    following = score(steps - 1, held_b)
    weigh(steps - 2, held_a, highest)
    give(steps - 2 - lag)
    weigh(steps - 1, held_b, following)
    give(steps - 1 - lag)
    for k in range(steps - lag, steps):
        give(k)

    for mask in range(GROUPS):
        landed(q_out, heads_here if mask else heads_here - 1, q_s.at[mask])
    landed(place_in, n - 1, p_s)
    landed(att_own, n, x_s)
    landed(mixed, n - 1, a_s)

    total = None
    for mask in (0, 1, 2, 3):
        g = plane_at(mask)
        landed(att_in, heads_here if mask else heads_here - 1, a_r.at[g])
        part = att_in[pl.ds(g * heads_here, heads_here)].reshape(cols, rows)
        term = jnp.dot(wo_turned[g], part, preferred_element_type=f32)
        total = term if total is None else total + term
    out_ref[...] = gate[...] * total


def whole_kernel(hidden, modulation, w_qkv, q_gain, k_gain, w_out, text_count, block_order):
    n = lax.axis_size("seq")
    states = hidden[0]
    rows, width = states.shape
    features = w_out.shape[0]
    cols = features // GROUPS
    half = width // 2
    wide = -(-half // LANES) * LANES
    bf, f32 = jnp.bfloat16, jnp.float32
    hbm = pl.BlockSpec(memory_space=pltpu.HBM)
    dma = pltpu.SemaphoreType.DMA
    turned = pl.pallas_call(
        functools.partial(fused, n),
        out_shape=jax.ShapeDtypeStruct((half, rows), f32),
        in_specs=[pl.BlockSpec(memory_space=pltpu.SMEM)] + [hbm] * 6,
        out_specs=pl.BlockSpec(memory_space=pltpu.VMEM),
        scratch_shapes=[
            pltpu.VMEM((rows, width), bf),
            pltpu.VMEM(modulation.shape, f32),
            pltpu.VMEM((1, HEAD), f32),
            pltpu.VMEM((1, HEAD), f32),
            pltpu.VMEM((3, GROUPS, width, cols), bf),
            pltpu.VMEM((features, wide), bf),
            pltpu.VMEM((GROUPS, half, cols), bf),
            pltpu.VMEM((half, rows), f32),
            pltpu.VMEM((rows, width), bf),
            pltpu.VMEM((n, 2 * HEAD, rows), bf),
            pltpu.VMEM((n, 2 * HEAD, rows), bf),
            pltpu.VMEM((n, HEAD, rows), bf),
            pltpu.VMEM((n, HEAD, rows), bf),
            pltpu.VMEM((1, 1, LANES), jnp.int32),
            pltpu.VMEM((n, 1, LANES), jnp.int32),
            pltpu.VMEM((n * rows // 2, 2 * LANES), bf),
            pltpu.VMEM((HEAD + 16, n * rows), bf),
        ] + [pltpu.VMEM((n, HEAD, rows), bf)] * 4 + [pltpu.VMEM((n * rows, 2 * rows), f32)] * 2 + [
            dma((4,)), dma((3, GROUPS)), dma,
            dma, dma, dma((GROUPS,)), dma((n,)), dma, dma, dma, dma((n // 2,)), dma, dma((GROUPS,)),
        ],
        compiler_params=pltpu.CompilerParams(
            collective_id=0, has_side_effects=True, vmem_limit_bytes=40 * 1024 * 1024),
    )(block_order * SHIFT + text_count, *[pltpu.with_memory_space_constraint(x, pltpu.HBM) for x in (
        states, modulation, w_qkv, q_gain[None], k_gain[None], w_out)])
    return turned.T


def solution(mesh):
    in_specs = (P("cfg", "seq", None), P(), P(), P(), P(), P(), P("cfg"), P("seq"))
    out_specs = P("seq", "cfg")
    one_head_each = mesh.shape["seq"] == HEADS and mesh.shape["cfg"] == 2
    body = whole_kernel if one_head_each else shards
    return jax.shard_map(body, mesh=mesh, in_specs=in_specs, out_specs=out_specs, check_vma=False)
```
